128 devices in a mesh: pod: 1, data: 64 (over z, y, x), stage: 2 (over core).
Axes of the slice: x: 4, y: 4, z: 4, core: 2. Of those that a mesh axis runs over, the one named last changes fastest.
Arguments:
- token_ids: int32 [128, 256], P(('pod', 'data'))
- label_ids: int32 [128, 256], P(('pod', 'data'))
- embed_table: bfloat16 [32128, 768], replicated
- w_up: bfloat16 [2, 768, 3072], P('stage')
- w_down: bfloat16 [2, 3072, 768], P('stage')
Outputs:
- output 1: float32 [128], P(('pod', 'data'))
- output 2: float32 [32128, 768], P(('pod', 'data'))
- output 3: float32 [2, 768, 3072], P(('pod', 'stage'), 'data')
- output 4: float32 [2, 3072, 768], P(('pod', 'stage'), 'data')
All inputs are finite; a program needn't handle non-finite values.
Results may differ from the reference program's by a relative error of at most 0.00717123.
Values are sent between devices in bfloat16 or wider.
A program may use at most 1 GiB of HBM per device.

```python
import jax
import jax.numpy as jnp
from jax import lax

VOCAB_SIZE = 32128
MODEL_DIM = 768
FFN_DIM = 3072
MICRO_BATCHES = 2
SEQ_TOKENS = 256
NUM_DATA = 64
NUM_STAGES = 2
HOT_IDS = 256
NORM_EPS = 1e-6


def draw_ids(key):
    key_pool, key_pick, key_wide, key_mix = jax.random.split(key, 4)
    shape_ids = (NUM_DATA * MICRO_BATCHES, SEQ_TOKENS + 1)
    hot_pool = jax.random.randint(key_pool, (HOT_IDS,), 0, VOCAB_SIZE)
    hot_ids = hot_pool[jax.random.randint(key_pick, shape_ids, 0, HOT_IDS)]
    wide_ids = jax.random.randint(key_wide, shape_ids, 0, VOCAB_SIZE)
    mixer = jax.random.randint(key_mix, shape_ids, 0, 2)
    stream = jnp.where(mixer == 0, hot_ids, wide_ids)
    stream = stream.at[0, :3].set(jnp.array([0, VOCAB_SIZE - 1, 0], jnp.int32))
    return stream[:, :-1], stream[:, 1:]


def setup_inputs(seed: int = 0, part: int = 0) -> dict:
    base_key = jax.random.key(seed)
    token_ids, label_ids = draw_ids(jax.random.fold_in(base_key, part))
    key_emb, key_one, key_two = jax.random.split(jax.random.fold_in(base_key, 1000003), 3)
    embed_table = jax.random.normal(key_emb, (VOCAB_SIZE, MODEL_DIM), jnp.float32).astype(jnp.bfloat16)
    w_up = (jax.random.normal(key_one, (NUM_STAGES, MODEL_DIM, FFN_DIM), jnp.float32) * MODEL_DIM ** -0.5).astype(jnp.bfloat16)
    w_down = (jax.random.normal(key_two, (NUM_STAGES, FFN_DIM, MODEL_DIM), jnp.float32) * FFN_DIM ** -0.5).astype(jnp.bfloat16)
    return {'token_ids': token_ids, 'label_ids': label_ids, 'embed_table': embed_table, 'w_up': w_up, 'w_down': w_down}


def stage_layer(state, w_one, w_two):
    wide = state.astype(jnp.float32)
    hidden = jnp.dot(wide, w_one)
    gated = jax.nn.gelu(hidden).astype(jnp.bfloat16)
    return (wide + jnp.dot(gated.astype(jnp.float32), w_two)).astype(jnp.bfloat16)


def token_ce(state, table, labels):
    wide = state.astype(jnp.float32)
    normed = (wide * lax.rsqrt(jnp.mean(wide * wide, axis=-1, keepdims=True) + NORM_EPS)).astype(jnp.bfloat16)
    logits = jnp.dot(normed.astype(jnp.float32), table.T) * (MODEL_DIM ** -0.5)
    picked = jnp.take_along_axis(logits, labels[:, None], axis=-1)[:, 0]
    return jax.nn.logsumexp(logits, axis=-1) - picked


def micro_objective(param_set, tokens, labels):
    table, stack_one, stack_two = param_set
    state = table[tokens].astype(jnp.bfloat16)

    def apply_layer(carry_state, weights):
        return stage_layer(carry_state, weights[0], weights[1]), None

    state, _ = lax.scan(apply_layer, state, (stack_one, stack_two))
    per_token = token_ce(state, table, labels)
    return jnp.sum(per_token), jnp.mean(per_token)


def reference(token_ids, label_ids, embed_table, w_up, w_down):
    params = (embed_table.astype(jnp.float32), w_up.astype(jnp.float32), w_down.astype(jnp.float32))

    def micro_step(grad_sum, batch):
        tokens, labels = batch
        total, pullback, mean_ce = jax.vjp(lambda param_set: micro_objective(param_set, tokens, labels), params, has_aux=True)
        grads = pullback(jnp.ones_like(total))[0]
        return jax.tree.map(lambda left, right: left + right, grad_sum, grads), mean_ce

    zeros = jax.tree.map(jnp.zeros_like, params)
    grad_sum, losses = lax.scan(micro_step, zeros, (token_ids, label_ids))
    return losses, grad_sum[0], grad_sum[1], grad_sum[2]
```

```python
import functools
import math

import jax
import jax.numpy as jnp
from jax import lax
from jax.experimental import pallas as pl
from jax.experimental.pallas import tpu as pltpu
from jax.sharding import PartitionSpec as P

NORM_EPS = 1e-6
BF = jnp.bfloat16
F32 = jnp.float32
VOCAB = 32128
DIM = 768
FFN = 3072
SEQ = 256
CHUNK = 768
NCH = FFN // CHUNK
ROWS = 502
WIN = 528
HALF = WIN // 2
SCALE = DIM ** -0.5
LOG2E = math.log2(math.e)
C2 = SCALE * LOG2E
GC = math.sqrt(2.0 / math.pi)
GA = 0.044715
VBLK = 2048
VSUB = 512
TBLK = 1024

NT = (((1,), (1,)), ((), ()))
NN = (((1,), (0,)), ((), ()))


def dot(a, b, dims):
    return lax.dot_general(a, b, dims, preferred_element_type=F32)


def gelu(h):
    return 0.5 * h * (1.0 + jnp.tanh(GC * (h + GA * h * h * h)))


def gelu_grad(h):
    t = jnp.tanh(GC * (h + GA * h * h * h))
    return 0.5 * (1.0 + t) + 0.5 * h * (1.0 - t * t) * (GC * (1.0 + 3.0 * GA * h * h))


def any_spec():
    return pl.BlockSpec(memory_space=pl.ANY)


def weight_copies(me, own_up, own_dn, oth_up, oth_dn, up_buf, dn_buf, sems):
    def up(ref, s, j):
        return pltpu.make_async_copy(ref.at[:, pl.ds(j * CHUNK, CHUNK)], up_buf.at[s, j], sems.at[s, j, 0])

    def dn(ref, s, j):
        return pltpu.make_async_copy(ref.at[pl.ds(j * CHUNK, CHUNK), :], dn_buf.at[s, j], sems.at[s, j, 1])

    def start(s, j):
        @pl.when(me == s)
        def _():
            up(own_up, s, j).start()
            dn(own_dn, s, j).start()

        @pl.when(me != s)
        def _():
            up(oth_up, s, j).start()
            dn(oth_dn, s, j).start()

    def wait(s, j):
        up(own_up, s, j).wait()
        dn(own_dn, s, j).wait()

    return start, wait


def fwd_kernel(me_ref, x_ref, own_up, own_dn, oth_up, oth_dn, x1_ref, x2_ref, n_ref, h_ref, up_buf, dn_buf, sems):
    start, wait = weight_copies(me_ref[0], own_up, own_dn, oth_up, oth_dn, up_buf, dn_buf, sems)
    for s in range(2):
        for j in range(NCH):
            start(s, j)
    x = x_ref[...]
    for s in range(2):
        acc = x.astype(F32)
        for j in range(NCH):
            wait(s, j)
            h = dot(x, up_buf[s, j], NN)
            h_ref[s, :, j * CHUNK:(j + 1) * CHUNK] = h
            acc = acc + dot(gelu(h).astype(BF), dn_buf[s, j], NN)
        x = acc.astype(BF)
        (x1_ref, x2_ref)[s][...] = x
    wide = x.astype(F32)
    inv = lax.rsqrt(jnp.mean(wide * wide, axis=-1, keepdims=True) + NORM_EPS)
    n_ref[...] = (wide * inv).astype(BF)


def bwd_kernel(me_ref, g_ref, h_ref, own_up, own_dn, oth_up, oth_dn, g1_ref, g0_ref, up_buf, dn_buf, sems):
    start, wait = weight_copies(me_ref[0], own_up, own_dn, oth_up, oth_dn, up_buf, dn_buf, sems)
    for s in (1, 0):
        for j in range(NCH):
            start(s, j)
    g = g_ref[...]
    for s in (1, 0):
        acc = g.astype(F32)
        for j in range(NCH):
            wait(s, j)
            gg = dot(g, dn_buf[s, j], NT).astype(BF).astype(F32)
            gh = (gg * gelu_grad(h_ref[s, :, j * CHUNK:(j + 1) * CHUNK])).astype(BF)
            acc = acc + dot(gh, up_buf[s, j], NT)
        g = acc.astype(BF)
        (g0_ref, g1_ref)[s][...] = g


def head_kernel(n_ref, lab_ref, el_ref, x2_ref, e_ref, gtop_ref, lse_ref, ce_ref, acc_ref, m_ref, s_ref, pk_ref):
    step = pl.program_id(0)
    last = pl.num_programs(0) - 1

    @pl.when(step == 0)
    def _():
        pk = jnp.sum(n_ref[...].astype(F32) * el_ref[...].astype(F32), axis=-1, keepdims=True) * C2
        pk_ref[...] = jnp.broadcast_to(pk, pk_ref.shape)
        m_ref[...] = jnp.broadcast_to(pk, m_ref.shape)
        s_ref[...] = jnp.zeros_like(s_ref)
        acc_ref[...] = jnp.zeros_like(acc_ref)

    def run(rows):
        n = n_ref[...]
        rel = lab_ref[...] - step * VBLK
        m = m_ref[:, :1]
        s = s_ref[:, :1]
        for lo in range(0, rows, VSUB):
            width = min(VSUB, rows - lo)
            e = e_ref[lo:lo + width, :]
            l = dot(n, e, NT)
            new = jnp.maximum(m, jnp.max(l, axis=-1, keepdims=True) * C2)
            p = jnp.exp2(l * C2 - new)
            hit = lax.broadcasted_iota(jnp.int32, (SEQ, width), 1) + lo == rel
            p = jnp.where(hit, 0.0, p)
            alpha = jnp.exp2(m - new)
            s = s * alpha + jnp.sum(p, axis=-1, keepdims=True)
            acc_ref[...] = acc_ref[...] * alpha + dot(p.astype(BF), e, NN)
            m = new
        m_ref[...] = jnp.broadcast_to(m, m_ref.shape)
        s_ref[...] = jnp.broadcast_to(s, s_ref.shape)

    @pl.when(step != last)
    def _():
        run(VBLK)

    @pl.when(step == last)
    def _():
        run(VOCAB % VBLK)
        m = m_ref[:, :1]
        s = s_ref[:, :1]
        pk = pk_ref[:, :1]
        total = s + jnp.exp2(pk - m)
        lse2 = m + jnp.log2(total)
        lse_ref[...] = lse2
        ce_ref[...] = (lse2 - pk) * (1.0 / LOG2E)
        inv_total = 1.0 / total
        gn = (acc_ref[...] * inv_total - (s * inv_total) * el_ref[...].astype(F32)) * SCALE
        gn = gn.astype(BF).astype(F32)
        wide = x2_ref[...].astype(F32)
        inv = lax.rsqrt(jnp.mean(wide * wide, axis=-1, keepdims=True) + NORM_EPS)
        nw = wide * inv
        inner = jnp.mean(gn * nw, axis=-1, keepdims=True)
        gtop_ref[...] = (inv * (gn - nw * inner)).astype(BF)


def headgrad_kernel(a_ref, table_ref, n_ref, lse_ref, lab_ref, out_ref, e_buf, sems):
    step = pl.program_id(0)

    def copy(seg):
        src = table_ref.at[pl.ds(pl.multiple_of(a_ref[seg], 16), WIN), :]
        return pltpu.make_async_copy(src, e_buf.at[seg], sems.at[seg])

    @pl.when(step == 0)
    def _():
        for seg in range(4):
            copy(seg).start()
        out_ref[...] = jnp.zeros_like(out_ref)
        for seg in range(4):
            copy(seg).wait()

    n = n_ref[...]
    lse = lse_ref[...] - math.log2(SCALE)
    lab = lab_ref[...]
    row = lax.broadcasted_iota(jnp.int32, (WIN, TBLK), 0)
    for seg in range(4):
        l = dot(e_buf[seg], n, NT)
        p = jnp.exp2(l * C2 - lse)
        g = (p - jnp.where(row == lab - a_ref[seg], SCALE, 0.0)).astype(BF)
        d = dot(g, n, NN)
        out_ref[0, seg] += d[:HALF]
        out_ref[1, seg] += d[HALF:]


def embgrad_kernel(a_ref, part_ref, g_ref, tok_ref, out_ref):
    step = pl.program_id(0)

    @pl.when(step == 0)
    def _():
        out_ref[...] = part_ref[...]

    g = g_ref[...]
    tok = tok_ref[...]
    row = lax.broadcasted_iota(jnp.int32, (WIN, TBLK), 0)
    for seg in range(4):
        hot = jnp.where(row == tok - a_ref[seg], 1.0, 0.0).astype(BF)
        d = dot(hot, g, NN)
        out_ref[0, seg] += d[:HALF]
        out_ref[1, seg] += d[HALF:]


def cost(flops, nbytes, trans=0):
    return pl.CostEstimate(flops=int(flops), bytes_accessed=int(nbytes), transcendentals=int(trans))


def call_fwd(me, x, own_up, own_dn, oth_up, oth_dn):
    tok = jax.ShapeDtypeStruct((SEQ, DIM), BF)
    return pl.pallas_call(
        fwd_kernel,
        out_shape=(tok, tok, tok, jax.ShapeDtypeStruct((2, SEQ, FFN), F32)),
        in_specs=[pl.BlockSpec(memory_space=pltpu.SMEM), pl.BlockSpec(memory_space=pltpu.VMEM)] + [any_spec()] * 4,
        out_specs=[pl.BlockSpec(memory_space=pltpu.VMEM)] * 4,
        scratch_shapes=[pltpu.VMEM((2, NCH, DIM, CHUNK), BF), pltpu.VMEM((2, NCH, CHUNK, DIM), BF), pltpu.SemaphoreType.DMA((2, NCH, 2))],
        cost_estimate=cost(8 * SEQ * DIM * FFN, 26e6),
        name='fwd')(me, x, own_up, own_dn, oth_up, oth_dn)


def call_bwd(me, g, h, own_up, own_dn, oth_up, oth_dn):
    tok = jax.ShapeDtypeStruct((SEQ, DIM), BF)
    return pl.pallas_call(
        bwd_kernel,
        out_shape=(tok, tok),
        in_specs=[pl.BlockSpec(memory_space=pltpu.SMEM)] + [pl.BlockSpec(memory_space=pltpu.VMEM)] * 2 + [any_spec()] * 4,
        out_specs=[pl.BlockSpec(memory_space=pltpu.VMEM)] * 2,
        scratch_shapes=[pltpu.VMEM((2, NCH, DIM, CHUNK), BF), pltpu.VMEM((2, NCH, CHUNK, DIM), BF), pltpu.SemaphoreType.DMA((2, NCH, 2))],
        cost_estimate=cost(8 * SEQ * DIM * FFN, 26e6),
        name='bwd')(me, g, h, own_up, own_dn, oth_up, oth_dn)


def call_head(n, lab, el, x2, table):
    full = lambda shape: pl.BlockSpec(shape, lambda i: (0, 0))
    return pl.pallas_call(
        head_kernel,
        grid=(pl.cdiv(VOCAB, VBLK),),
        out_shape=(jax.ShapeDtypeStruct((SEQ, DIM), BF), jax.ShapeDtypeStruct((SEQ, 1), F32), jax.ShapeDtypeStruct((SEQ, 1), F32)),
        in_specs=[full((SEQ, DIM)), full((SEQ, 1)), full((SEQ, DIM)), full((SEQ, DIM)), pl.BlockSpec((VBLK, DIM), lambda i: (i, 0))],
        out_specs=(full((SEQ, DIM)), full((SEQ, 1)), full((SEQ, 1))),
        scratch_shapes=[pltpu.VMEM((SEQ, DIM), F32)] + [pltpu.VMEM((SEQ, 128), F32)] * 3,
        cost_estimate=cost(4 * SEQ * DIM * VOCAB, VOCAB * DIM * 2, SEQ * VOCAB),
        name='head')(n, lab, el, x2, table)


def call_headgrad(starts, table, n_all, lse_all, lab_all):
    toks = n_all.shape[0]
    return pl.pallas_call(
        headgrad_kernel,
        grid=(toks // TBLK,),
        out_shape=jax.ShapeDtypeStruct((2, 4, HALF, DIM), F32),
        in_specs=[pl.BlockSpec(memory_space=pltpu.SMEM), any_spec(), pl.BlockSpec((TBLK, DIM), lambda i: (i, 0)),
                  pl.BlockSpec((1, TBLK), lambda i: (0, i)), pl.BlockSpec((1, TBLK), lambda i: (0, i))],
        out_specs=pl.BlockSpec((2, 4, HALF, DIM), lambda i: (0, 0, 0, 0)),
        scratch_shapes=[pltpu.VMEM((4, WIN, DIM), BF), pltpu.SemaphoreType.DMA((4,))],
        cost_estimate=cost(4 * 4 * WIN * DIM * toks, 16e6, 4 * WIN * toks),
        name='headgrad')(starts, table, n_all, lse_all, lab_all)


def call_embgrad(starts, part, g_all, tok_all):
    toks = g_all.shape[0]
    shape = (2, 4, HALF, DIM)
    return pl.pallas_call(
        embgrad_kernel,
        grid=(toks // TBLK,),
        out_shape=jax.ShapeDtypeStruct(shape, F32),
        in_specs=[pl.BlockSpec(memory_space=pltpu.SMEM), pl.BlockSpec(shape, lambda i: (0, 0, 0, 0)),
                  pl.BlockSpec((TBLK, DIM), lambda i: (i, 0)), pl.BlockSpec((1, TBLK), lambda i: (0, i))],
        out_specs=pl.BlockSpec(shape, lambda i: (0, 0, 0, 0)),
        cost_estimate=cost(2 * 4 * WIN * DIM * toks, 20e6),
        name='embgrad')(starts, part, g_all, tok_all)


SWAP = [(0, 1), (1, 0)]


def gather_z(v):
    parts = [v]
    for k in (1, 3, 2):
        parts.append(lax.ppermute(v, 'z', [(i, (i + k) % 4) for i in range(4)]))
    return jnp.concatenate(parts, axis=0)


def step_program(token_rows, label_rows, table, up_block, down_block):
    me = lax.axis_index('stage')
    iz, iy, ix = lax.axis_index('z'), lax.axis_index('y'), lax.axis_index('x')
    own_up, own_dn = up_block[0], down_block[0]
    oth_up = lax.ppermute(own_up, 'stage', SWAP)
    oth_dn = lax.ppermute(own_dn, 'stage', SWAP)
    me1 = me.reshape(1).astype(jnp.int32)
    tok = lax.dynamic_index_in_dim(token_rows, me, 0, keepdims=False)
    lab = lax.dynamic_index_in_dim(label_rows, me, 0, keepdims=False)
    rows = table[jnp.concatenate([tok, lab])]
    x0, el = rows[:SEQ], rows[SEQ:]
    x1, x2, n, h = call_fwd(me1, x0, own_up, own_dn, oth_up, oth_dn)
    n_all = lax.all_gather(n, ('y', 'x'), axis=0, tiled=True)
    x_own = jnp.where(me == 0, x0, x1)
    x_oth = lax.ppermute(jnp.where(me == 0, x1, x0), 'stage', SWAP)
    x_g = gather_z(jnp.concatenate([x_own, x_oth], axis=0))
    gtop, lse, ce = call_head(n, lab[:, None], el, x2, table)
    g1, g0 = call_bwd(me1, gtop, h, own_up, own_dn, oth_up, oth_dn)
    g_all = lax.all_gather(g0, ('y', 'x'), axis=0, tiled=True)
    small = jnp.stack([lse[:, 0], lab.astype(F32), tok.astype(F32)])
    small = lax.all_gather(small, ('y', 'x'), axis=1, tiled=True)
    lse_all = small[0:1]
    lab_all = small[1:2].astype(jnp.int32)
    tok_all = small[2:3].astype(jnp.int32)

    owner = (jnp.arange(4, dtype=jnp.int32) * 4 + iy) * 4 + ix
    starts = jnp.minimum(owner * ROWS // 16 * 16, VOCAB - WIN)
    part = call_headgrad(starts, table, n_all, lse_all, lab_all)

    go_own = jnp.where(me == 0, g1, gtop)
    go_oth = lax.ppermute(jnp.where(me == 0, gtop, g1), 'stage', SWAP)
    go_g = gather_z(jnp.concatenate([go_own, go_oth], axis=0))
    up_sl = lax.dynamic_slice_in_dim(own_up, iz * CHUNK, CHUNK, 1)
    dn_sl = lax.dynamic_slice_in_dim(own_dn, iz * CHUNK, CHUNK, 0)
    hid = dot(x_g, up_sl, NN)
    gg = dot(go_g, dn_sl, NT).astype(BF).astype(F32)
    gated = gelu(hid).astype(BF)
    gh = (gg * gelu_grad(hid)).astype(BF)
    d_dn = lax.dot_general(gated, go_g, (((0,), (0,)), ((), ())), preferred_element_type=F32)
    d_up = lax.dot_general(x_g, gh, (((0,), (0,)), ((), ())), preferred_element_type=F32)
    d_up = d_up.reshape(4, 16, 12, CHUNK).transpose(1, 0, 2, 3).reshape(16, 48, CHUNK)
    d_w = jnp.concatenate([d_up, d_dn.reshape(16, 48, DIM)], axis=1).reshape(16 * 96, DIM)
    d_w = lax.psum_scatter(d_w, ('y', 'x'), scatter_dimension=0, tiled=True)
    grad_down = d_w[48:][None]
    up_parts = lax.all_to_all(d_w[:48].reshape(4, 12, CHUNK), 'z', split_axis=0, concat_axis=0, tiled=True)
    grad_up = up_parts.transpose(1, 0, 2).reshape(1, 12, FFN)

    part = call_embgrad(starts, part, g_all, tok_all)
    part = lax.psum_scatter(part, 'stage', scatter_dimension=0, tiled=True)[0]
    mine = lax.psum_scatter(part, 'z', scatter_dimension=0, tiled=True)[0]
    both = lax.all_gather(mine, 'stage', axis=0, tiled=True)
    my_owner = (iz * 4 + iy) * 4 + ix
    my_start = jnp.minimum(my_owner * ROWS // 16 * 16, VOCAB - WIN)
    grad_table = lax.dynamic_slice_in_dim(both, my_owner * ROWS - my_start, ROWS, 0)

    loss = jnp.mean(ce).reshape(1)
    losses = lax.all_gather(loss, 'stage', axis=0, tiled=True)
    return losses, grad_table, grad_up, grad_down


def solution(mesh):
    fine = jax.sharding.Mesh(mesh.devices.reshape(1, 4, 4, 4, 2), ('pod', 'z', 'y', 'x', 'stage'))
    data = ('z', 'y', 'x')
    rows_spec = P(('pod',) + data, None)
    return jax.shard_map(step_program, mesh=fine,
                         in_specs=(rows_spec, rows_spec, P(None, None), P('stage', None, None), P('stage', None, None)),
                         out_specs=(P(('pod',) + data), rows_spec, P(('pod', 'stage'), data, None), P(('pod', 'stage'), data, None)),
                         check_vma=False)
```

```python
import functools
import math

import jax
import jax.numpy as jnp
from jax import lax
from jax.experimental import pallas as pl
from jax.experimental.pallas import tpu as pltpu
from jax.sharding import PartitionSpec as P

NORM_EPS = 1e-6
BF = jnp.bfloat16
F32 = jnp.float32
VOCAB = 32128
DIM = 768
FFN = 3072
SEQ = 256
CHUNK = 768
NCH = FFN // CHUNK
ROWS = 502
WIN = 528
HALF = WIN // 2
SCALE = DIM ** -0.5
LOG2E = math.log2(math.e)
C2 = SCALE * LOG2E
GC = math.sqrt(2.0 / math.pi)
GA = 0.044715
VBLK = 2048
VSUB = 512
TBLK = 1024
VSTEPS = -(-VOCAB // VBLK)
HBLK = 512
HSTEPS = 16 * SEQ // HBLK
SPLIT = 136
AXES = ('pod', 'z', 'y', 'x', 'stage')

NT = (((1,), (1,)), ((), ()))
NN = (((1,), (0,)), ((), ()))
TN = (((0,), (0,)), ((), ()))


def dot(a, b, dims):
    return lax.dot_general(a, b, dims, preferred_element_type=F32)


def gelu(h):
    return 0.5 * h * (1.0 + jnp.tanh(GC * (h + GA * h * h * h)))


def gelu_grad(h):
    t = jnp.tanh(GC * (h + GA * h * h * h))
    return 0.5 * (1.0 + t) + 0.5 * h * (1.0 - t * t) * (GC * (1.0 + 3.0 * GA * h * h))


def any_spec():
    return pl.BlockSpec(memory_space=pl.ANY)


def weight_copies(me, own_up, own_dn, oth_up, oth_dn, up_buf, dn_buf, sems):
    def up(ref, s, j):
        return pltpu.make_async_copy(ref.at[:, pl.ds(j * CHUNK, CHUNK)], up_buf.at[s, j], sems.at[s, j, 0])

    def dn(ref, s, j):
        return pltpu.make_async_copy(ref.at[pl.ds(j * CHUNK, CHUNK), :], dn_buf.at[s, j], sems.at[s, j, 1])

    def start(s, j):
        @pl.when(me == s)
        def _():
            up(own_up, s, j).start()
            dn(own_dn, s, j).start()

        @pl.when(me != s)
        def _():
            up(oth_up, s, j).start()
            dn(oth_dn, s, j).start()

    def wait(s, j):
        up(own_up, s, j).wait()
        dn(own_dn, s, j).wait()

    return start, wait


def fwd_kernel(x_ref, own_up, own_dn, oth_up, oth_dn, xs_ref, x2_ref, n_ref, h_ref, up_buf, dn_buf, sems):
    start, wait = weight_copies(lax.axis_index('stage'), own_up, own_dn, oth_up, oth_dn, up_buf, dn_buf, sems)
    for s in range(2):
        for j in range(NCH):
            start(s, j)
    x = x_ref[...]
    for s in range(2):
        xs_ref[s] = x
        acc = x.astype(F32)
        for j in range(NCH):
            wait(s, j)
            h = dot(x, up_buf[s, j], NN)
            h_ref[s, :, j * CHUNK:(j + 1) * CHUNK] = h
            acc = acc + dot(gelu(h).astype(BF), dn_buf[s, j], NN)
        x = acc.astype(BF)
    x2_ref[...] = x
    wide = x.astype(F32)
    inv = lax.rsqrt(jnp.mean(wide * wide, axis=-1, keepdims=True) + NORM_EPS)
    n_ref[...] = (wide * inv).astype(BF)


def mod4(i):
    return lax.rem(i + 8, 4)


def ident(**kw):
    base = {name: lax.axis_index(name) for name in AXES}
    base.update(kw)
    return tuple(base[name] for name in AXES)


def remote(src, dst, send, recv, **kw):
    return pltpu.make_async_remote_copy(src_ref=src, dst_ref=dst, send_sem=send, recv_sem=recv, device_id=ident(**kw),
                                        device_id_type=pl.DeviceIdType.MESH)


def greet(targets):
    barrier = pltpu.get_barrier_semaphore()
    for kw in targets:
        pl.semaphore_signal(barrier, inc=1, device_id=ident(**kw), device_id_type=pl.DeviceIdType.MESH)
    pl.semaphore_wait(barrier, len(targets))


def bwd_kernel(g_ref, h_ref, small_ref, own_up, own_dn, oth_up, oth_dn, go_ref, g0_ref, all_ref, up_buf, dn_buf, sems, send, recv):
    me = lax.axis_index('stage')
    iy, ix = lax.axis_index('y'), lax.axis_index('x')
    start, wait = weight_copies(me, own_up, own_dn, oth_up, oth_dn, up_buf, dn_buf, sems)
    for s in (1, 0):
        for j in range(NCH):
            start(s, j)
    peers = [dict(y=mod4(iy + k // 4), x=mod4(ix + k % 4)) for k in range(1, 16)]
    greet(peers)
    slot = iy * 4 + ix
    copies = [remote(small_ref, all_ref.at[slot], send.at[k], recv.at[k], **kw) for k, kw in enumerate(peers)]
    for copy in copies:
        copy.start()
    g = g_ref[...]
    for s in (1, 0):
        go_ref[s] = g
        acc = g.astype(F32)
        for j in range(NCH):
            wait(s, j)
            gg = dot(g, dn_buf[s, j], NT).astype(BF).astype(F32)
            gh = (gg * gelu_grad(h_ref[s, :, j * CHUNK:(j + 1) * CHUNK])).astype(BF)
            acc = acc + dot(gh, up_buf[s, j], NT)
        g = acc.astype(BF)
    g0_ref[...] = g
    all_ref[slot] = small_ref[...]
    for copy in copies:
        copy.wait()


class ZGather:
    def __init__(self, src, dst, local, send, recv):
        me, iz = lax.axis_index('stage'), lax.axis_index('z')
        up, down = mod4(iz + 1), mod4(iz - 1)
        self.targets = [dict(stage=1 - me), dict(z=up), dict(z=down)]
        self.own = pltpu.make_async_copy(src.at[me], dst.at[iz, me], local)
        self.swap = remote(src.at[1 - me], dst.at[iz, me], send.at[0], recv.at[0], stage=1 - me)
        self.first = [remote(dst.at[iz], dst.at[iz], send.at[1], recv.at[1], z=up),
                      remote(dst.at[iz], dst.at[iz], send.at[2], recv.at[2], z=down)]
        self.second = [remote(dst.at[down, 0], dst.at[down, 0], send.at[3], recv.at[3], z=up),
                       remote(dst.at[up, 1], dst.at[up, 1], send.at[4], recv.at[4], z=down)]

    def begin(self):
        greet(self.targets)
        self.swap.start()
        self.own.start()

    def spread(self):
        self.swap.wait()
        self.own.wait()
        for copy in self.first:
            copy.start()

    def forward(self):
        for copy in self.first:
            copy.wait()
        for copy in self.second:
            copy.start()

    def end(self):
        for copy in self.second:
            copy.wait()


def head_kernel(n_ref, lab_ref, ids_ref, el_ref, x2_ref, xs_ref, e_ref, gtop_ref, small_ref, ce_ref, xg_ref,
                acc_ref, m_ref, s_ref, pk_ref, local, send, recv):
    step = pl.program_id(0)
    last = VSTEPS - 1
    gather = ZGather(xs_ref, xg_ref, local, send, recv)

    @pl.when(step == 0)
    def _():
        gather.begin()

    @pl.when(step == 2)
    def _():
        gather.spread()

    @pl.when(step == 9)
    def _():
        gather.forward()

    @pl.when(step == 0)
    def _():
        pk = jnp.sum(n_ref[...].astype(F32) * el_ref[...].astype(F32), axis=-1, keepdims=True) * C2
        pk_ref[...] = jnp.broadcast_to(pk, pk_ref.shape)
        m_ref[...] = jnp.broadcast_to(pk, m_ref.shape)
        s_ref[...] = jnp.zeros_like(s_ref)
        acc_ref[...] = jnp.zeros_like(acc_ref)

    def run(rows):
        n = n_ref[...]
        rel = lab_ref[...] - step * VBLK
        m = m_ref[:, :1]
        s = s_ref[:, :1]
        for lo in range(0, rows, VSUB):
            width = min(VSUB, rows - lo)
            e = e_ref[lo:lo + width, :]
            l = dot(n, e, NT)
            new = jnp.maximum(m, jnp.max(l, axis=-1, keepdims=True) * C2)
            p = jnp.exp2(l * C2 - new)
            hit = lax.broadcasted_iota(jnp.int32, (SEQ, width), 1) + lo == rel
            p = jnp.where(hit, 0.0, p)
            alpha = jnp.exp2(m - new)
            s = s * alpha + jnp.sum(p, axis=-1, keepdims=True)
            acc_ref[...] = acc_ref[...] * alpha + dot(p.astype(BF), e, NN)
            m = new
        m_ref[...] = jnp.broadcast_to(m, m_ref.shape)
        s_ref[...] = jnp.broadcast_to(s, s_ref.shape)

    @pl.when(step != last)
    def _():
        run(VBLK)

    @pl.when(step == last)
    def _():
        run(VOCAB % VBLK)
        m = m_ref[:, :1]
        s = s_ref[:, :1]
        pk = pk_ref[:, :1]
        total = s + jnp.exp2(pk - m)
        lse2 = m + jnp.log2(total)
        lse_rows = jnp.transpose(jnp.broadcast_to(lse2, (SEQ, 128)))[:8]
        row = lax.broadcasted_iota(jnp.int32, (8, SEQ), 0)
        small_ref[...] = jnp.where(row == 0, lse_rows, ids_ref[...])
        ce_ref[...] = (lse2 - pk) * (1.0 / LOG2E)
        inv_total = 1.0 / total
        gn = (acc_ref[...] * inv_total - (s * inv_total) * el_ref[...].astype(F32)) * SCALE
        gn = gn.astype(BF).astype(F32)
        wide = x2_ref[...].astype(F32)
        inv = lax.rsqrt(jnp.mean(wide * wide, axis=-1, keepdims=True) + NORM_EPS)
        nw = wide * inv
        inner = jnp.mean(gn * nw, axis=-1, keepdims=True)
        gtop_ref[...] = (inv * (gn - nw * inner)).astype(BF)
        gather.end()


def window_start(seg):
    owner = (seg * 4 + lax.axis_index('y')) * 4 + lax.axis_index('x')
    return jnp.minimum(owner * ROWS // 16 * 16, VOCAB - WIN)


def headgrad_kernel(table_ref, n_ref, all_ref, go_ref, out_ref, gg_ref, e_buf, sems, local, send, recv):
    step = pl.program_id(0)
    gather = ZGather(go_ref, gg_ref, local, send, recv)

    def copy(seg):
        src = table_ref.at[pl.ds(pl.multiple_of(window_start(seg), 16), WIN), :]
        return pltpu.make_async_copy(src, e_buf.at[seg], sems.at[seg])

    @pl.when(step == 0)
    def _():
        for seg in range(4):
            copy(seg).start()
        gather.begin()
        out_ref[...] = jnp.zeros_like(out_ref)
        for seg in range(4):
            copy(seg).wait()

    @pl.when(step == 1)
    def _():
        gather.spread()

    @pl.when(step == HSTEPS - 2)
    def _():
        gather.forward()

    n = n_ref[...]
    lse = jnp.concatenate([all_ref[q, 0:1, :] for q in range(HBLK // SEQ)], axis=1) - math.log2(SCALE)
    lab = jnp.concatenate([all_ref[q, 1:2, :] for q in range(HBLK // SEQ)], axis=1).astype(jnp.int32)
    row = lax.broadcasted_iota(jnp.int32, (WIN, HBLK), 0)
    for seg in range(4):
        l = dot(e_buf[seg], n, NT)
        p = jnp.exp2(l * C2 - lse)
        g = (p - jnp.where(row == lab - window_start(seg), SCALE, 0.0)).astype(BF)
        d = dot(g, n, NN)
        out_ref[seg, 0] += d[:HALF]
        out_ref[seg, 1] += d[HALF:]

    @pl.when(step == HSTEPS - 1)
    def _():
        gather.end()


def wgrad_kernel(*refs):
    x_refs, g_refs = refs[0:4], refs[4:8]
    up_ref, dn_ref, out_up, out_dn, wu, wd, acc_up, acc_dn, sems = refs[8:]
    iz = lax.axis_index('z')
    first = pl.multiple_of(iz * CHUNK, CHUNK)
    cu = pltpu.make_async_copy(up_ref.at[:, pl.ds(first, CHUNK)], wu, sems.at[0])
    cd = pltpu.make_async_copy(dn_ref.at[pl.ds(first, CHUNK), :], wd, sems.at[1])
    cu.start()
    cd.start()
    cu.wait()
    cd.wait()
    for q in range(4):
        x = x_refs[q][0].reshape(2 * SEQ, DIM)
        g = g_refs[q][0].reshape(2 * SEQ, DIM)
        hid = dot(x, wu[...], NN)
        gg = dot(g, wd[...], NT).astype(BF).astype(F32)
        gated = gelu(hid).astype(BF)
        gh = (gg * gelu_grad(hid)).astype(BF)
        du = dot(x, gh, TN)
        dd = dot(gated, g, TN)
        if q == 0:
            acc_up[...] = du
            acc_dn[...] = dd
        else:
            acc_up[...] += du
            acc_dn[...] += dd
    for k in range(64):
        kz, ky, kx = k // 16, k // 4 % 4, k % 4
        out_up[kx, ky, 12 * kz:12 * kz + 12, :] = acc_up[12 * k:12 * k + 12, :]
    for k in range(16):
        out_dn[k // 4, k % 4] = acc_dn[48 * k:48 * k + 48, :]


class PlaneReduce:
    def __init__(self, src, first, second, bufs, sems):
        self.src, self.bufs, self.sems = src, bufs, sems
        self.first, self.second = first, second

    def axis(self, name):
        i = lax.axis_index(name)
        return i, mod4(i + 1), mod4(i - 1), mod4(i + 2)

    def sem(self, k):
        return self.sems.at[0, k], self.sems.at[1, k]

    def pieces(self, phase):
        rel1, fin1, snd1, total, rel2, fin2, snd2 = self.bufs
        if phase == 0:
            name, src, rel, fin, snd, half, base = self.first, self.src, rel1, fin1, snd1, 2, 0
        else:
            name, src, rel, fin, snd, half, base = self.second, total, rel2, fin2, snd2, 24, 6
        i, up, down, far = self.axis(name)
        lo, hi = pl.ds(0, half), pl.ds(half, half)
        to_up, to_down = {name: up}, {name: down}
        early = [remote(src.at[far, lo], rel.at[0], *self.sem(base), **to_up),
                 remote(src.at[far, hi], rel.at[1], *self.sem(base + 1), **to_down),
                 remote(src.at[up, hi], fin.at[0, hi], *self.sem(base + 2), **to_up),
                 remote(src.at[down, lo], fin.at[1, lo], *self.sem(base + 3), **to_down)]
        late = [remote(snd.at[0], fin.at[0, lo], *self.sem(base + 4), **to_up),
                remote(snd.at[1], fin.at[1, hi], *self.sem(base + 5), **to_down)]
        return i, up, down, lo, hi, src, rel, fin, snd, early, late

    def start(self, phase):
        for copy in self.pieces(phase)[-2]:
            copy.start()

    def relay(self, phase):
        i, up, down, lo, hi, src, rel, fin, snd, early, late = self.pieces(phase)
        early[0].wait_recv()
        snd[0] = src[up, lo] + rel[0]
        late[0].start()
        early[1].wait_recv()
        snd[1] = src[down, hi] + rel[1]
        late[1].start()

    def finish(self, phase):
        i, up, down, lo, hi, src, rel, fin, snd, early, late = self.pieces(phase)
        for copy in early[2:] + late:
            copy.wait_recv()
        return src[i] + fin[0] + fin[1]

    def drain(self, phase):
        early, late = self.pieces(phase)[-2:]
        for copy in early + late:
            copy.wait_send()


def final_kernel(part_ref, g_ref, all_ref, up_ref, dn_ref, tab_ref, upo_ref, dno_ref,
                 t_ref, swap_ref, zrel0, zrel1, zfin, mine, theirs, u4, ugot, *rest):
    bufs_a, bufs_b = rest[0:7], rest[7:14]
    sems_a, sems_b, sems_c, sems_z, sems_u, sems_f = rest[14:]
    me, iz, iy, ix = (lax.axis_index(name) for name in ('stage', 'z', 'y', 'x'))
    up, down, far = mod4(iz + 1), mod4(iz - 1), mod4(iz + 2)
    greet([dict(stage=1 - me), dict(z=up), dict(z=down), dict(z=far), dict(y=mod4(iy + 1)), dict(y=mod4(iy - 1)),
           dict(x=mod4(ix + 1)), dict(x=mod4(ix - 1))])
    red_a = PlaneReduce(up_ref, 'x', 'y', bufs_a, sems_a)
    red_b = PlaneReduce(dn_ref, 'y', 'x', bufs_b, sems_b)
    red_a.start(0)
    red_b.start(0)
    total_a, total_b = bufs_a[3], bufs_b[3]
    order = (far, up, down, iz)
    swaps = [remote(t_ref.at[seg, 1 - me], swap_ref.at[k], sems_c.at[0, k], sems_c.at[1, k], stage=1 - me) for k, seg in enumerate(order)]
    lo, hi = pl.ds(0, SPLIT), pl.ds(SPLIT, HALF - SPLIT)

    def zsem(k):
        return sems_z.at[0, k], sems_z.at[1, k]

    rel_up = remote(t_ref.at[far, me, lo], zrel0, *zsem(0), z=up)
    rel_down = remote(t_ref.at[far, me, hi], zrel1, *zsem(1), z=down)
    up_hi = remote(t_ref.at[up, me, hi], zfin.at[0, hi], *zsem(2), z=up)
    up_lo = remote(t_ref.at[up, me, lo], zfin.at[0, lo], *zsem(3), z=up)
    down_lo = remote(t_ref.at[down, me, lo], zfin.at[1, lo], *zsem(4), z=down)
    down_hi = remote(t_ref.at[down, me, hi], zfin.at[1, hi], *zsem(5), z=down)

    def embed(seg):
        row = lax.broadcasted_iota(jnp.int32, (WIN, TBLK), 0)
        for b in range(4):
            tok = jnp.concatenate([all_ref[4 * b + q, 2:3, :] for q in range(4)], axis=1).astype(jnp.int32)
            hot = jnp.where(row == tok - window_start(seg), 1.0, 0.0).astype(BF)
            d = dot(hot, g_ref[b * TBLK:(b + 1) * TBLK, :], NN)
            base = part_ref if b == 0 else t_ref
            t_ref[seg, 0] = base[seg, 0] + d[:HALF]
            t_ref[seg, 1] = base[seg, 1] + d[HALF:]

    def merge(k):
        swaps[k].wait_recv()
        t_ref[order[k], me] += swap_ref[k]

    embed(far)
    swaps[0].start()
    embed(up)
    merge(0)
    rel_up.start()
    rel_down.start()
    swaps[1].start()
    red_a.relay(0)
    red_b.relay(0)
    embed(down)
    merge(1)
    up_hi.start()
    swaps[2].start()
    embed(iz)
    merge(2)
    down_lo.start()
    swaps[3].start()
    rel_up.wait_recv()
    t_ref[up, me, lo] += zrel0[...]
    up_lo.start()
    rel_down.wait_recv()
    t_ref[down, me, hi] += zrel1[...]
    down_hi.start()
    total_a[...] = red_a.finish(0)
    red_a.start(1)
    total_b[...] = red_b.finish(0)
    red_b.start(1)
    swaps[3].wait_recv()
    red_a.relay(1)
    red_b.relay(1)
    whole = red_a.finish(1)
    for k in range(4):
        u4[k] = whole[12 * k:12 * k + 12, :]
    turns = [remote(u4.at[mod4(iz + k)], ugot.at[iz], sems_u.at[0, k - 1], sems_u.at[1, k - 1], z=mod4(iz + k)) for k in (1, 2, 3)]
    for copy in turns:
        copy.start()
    dno_ref[...] = red_b.finish(1)
    for copy in (up_hi, up_lo, down_lo, down_hi):
        copy.wait_recv()
    mine[...] = t_ref[iz, me] + swap_ref[3] + zfin[0] + zfin[1]
    back = remote(mine, theirs, sems_f.at[0], sems_f.at[1], stage=1 - me)
    back.start()
    tab_ref[me] = mine[...]
    for copy in turns:
        copy.wait_recv()
    upo_ref[...] = ugot[...]
    upo_ref[iz] = u4[iz]
    back.wait_recv()
    tab_ref[1 - me] = theirs[...]
    for copy in swaps + [rel_up, rel_down, up_hi, up_lo, down_lo, down_hi, back] + turns:
        copy.wait_send()
    for phase in (0, 1):
        red_a.drain(phase)
        red_b.drain(phase)


def cost(flops, nbytes, trans=0):
    return pl.CostEstimate(flops=int(flops), bytes_accessed=int(nbytes), transcendentals=int(trans))


def vmem(n):
    return [pl.BlockSpec(memory_space=pltpu.VMEM)] * n


def shape(dims, dtype=F32):
    return jax.ShapeDtypeStruct(dims, dtype)


def comm(cid):
    return pltpu.CompilerParams(collective_id=cid, has_side_effects=True)


WBUFS = [pltpu.VMEM((2, NCH, DIM, CHUNK), BF), pltpu.VMEM((2, NCH, CHUNK, DIM), BF), pltpu.SemaphoreType.DMA((2, NCH, 2))]
GSEMS = [pltpu.SemaphoreType.DMA, pltpu.SemaphoreType.DMA((5,)), pltpu.SemaphoreType.DMA((5,))]


def call_fwd(x, *weights):
    tok = shape((SEQ, DIM), BF)
    return pl.pallas_call(
        fwd_kernel,
        out_shape=(shape((2, SEQ, DIM), BF), tok, tok, shape((2, SEQ, FFN))),
        in_specs=vmem(1) + [any_spec()] * 4,
        out_specs=vmem(4),
        scratch_shapes=WBUFS,
        cost_estimate=cost(8 * SEQ * DIM * FFN, 26e6),
        name='fwd')(x, *weights)


def call_bwd(g, h, small, *weights):
    return pl.pallas_call(
        bwd_kernel,
        out_shape=(shape((2, SEQ, DIM), BF), shape((SEQ, DIM), BF), shape((16, 8, SEQ))),
        in_specs=vmem(3) + [any_spec()] * 4,
        out_specs=vmem(3),
        scratch_shapes=WBUFS + [pltpu.SemaphoreType.DMA((15,)), pltpu.SemaphoreType.DMA((15,))],
        compiler_params=comm(1),
        cost_estimate=cost(8 * SEQ * DIM * FFN, 26e6),
        name='bwd')(g, h, small, *weights)


def call_head(n, lab, ids, el, x2, xs, table):
    full = lambda dims: pl.BlockSpec(dims, lambda i: (0,) * len(dims))
    return pl.pallas_call(
        head_kernel,
        grid=(VSTEPS,),
        out_shape=(shape((SEQ, DIM), BF), shape((8, SEQ)), shape((SEQ, 1)), shape((4, 2, SEQ, DIM), BF)),
        in_specs=[full((SEQ, DIM)), full((SEQ, 1)), full((8, SEQ)), full((SEQ, DIM)), full((SEQ, DIM)), any_spec(),
                  pl.BlockSpec((VBLK, DIM), lambda i: (i, 0))],
        out_specs=(full((SEQ, DIM)), full((8, SEQ)), full((SEQ, 1)), any_spec()),
        scratch_shapes=[pltpu.VMEM((SEQ, DIM), F32)] + [pltpu.VMEM((SEQ, 128), F32)] * 3 + GSEMS,
        compiler_params=comm(2),
        cost_estimate=cost(4 * SEQ * DIM * VOCAB, VOCAB * DIM * 2, SEQ * VOCAB),
        name='head')(n, lab, ids, el, x2, xs, table)


def call_headgrad(table, n_all, small_all, go):
    toks = n_all.shape[0]
    return pl.pallas_call(
        headgrad_kernel,
        grid=(HSTEPS,),
        out_shape=(shape((4, 2, HALF, DIM)), shape((4, 2, SEQ, DIM), BF)),
        in_specs=[any_spec(), pl.BlockSpec((HBLK, DIM), lambda i: (i, 0)), pl.BlockSpec((HBLK // SEQ, 8, SEQ), lambda i: (i, 0, 0)), any_spec()],
        out_specs=(pl.BlockSpec((4, 2, HALF, DIM), lambda i: (0, 0, 0, 0)), any_spec()),
        scratch_shapes=[pltpu.VMEM((4, WIN, DIM), BF), pltpu.SemaphoreType.DMA((4,))] + GSEMS,
        compiler_params=comm(3),
        cost_estimate=cost(4 * 4 * WIN * DIM * toks, 16e6, 4 * WIN * toks),
        name='headgrad')(table, n_all, small_all, go)


def call_wgrad(xg, gg, own_up, own_dn):
    block = lambda q: pl.BlockSpec((1, 2, SEQ, DIM), lambda i, q=q: (q, 0, 0, 0))
    res = pl.BlockSpec((4, 4, 48, DIM), lambda i: (0, 0, 0, 0))
    return pl.pallas_call(
        wgrad_kernel,
        grid=(1,),
        out_shape=(shape((4, 4, 48, DIM)), shape((4, 4, 48, DIM))),
        in_specs=[block(q) for q in range(4)] * 2 + [any_spec()] * 2,
        out_specs=(res, res),
        scratch_shapes=[pltpu.VMEM((DIM, CHUNK), BF), pltpu.VMEM((CHUNK, DIM), BF), pltpu.VMEM((DIM, CHUNK), F32),
                        pltpu.VMEM((CHUNK, DIM), F32), pltpu.SemaphoreType.DMA((2,))],
        cost_estimate=cost(8 * 2048 * DIM * CHUNK, 16e6),
        name='wgrad')(*([xg] * 4), *([gg] * 4), own_up, own_dn)


def plane_bufs():
    return [pltpu.VMEM((2, 2, 48, DIM), F32), pltpu.VMEM((2, 4, 48, DIM), F32), pltpu.VMEM((2, 2, 48, DIM), F32),
            pltpu.VMEM((4, 48, DIM), F32), pltpu.VMEM((2, 24, DIM), F32), pltpu.VMEM((2, 48, DIM), F32), pltpu.VMEM((2, 24, DIM), F32)]


def call_final(part, g_all, small_all, d_up, d_dn):
    dma = pltpu.SemaphoreType.DMA
    return pl.pallas_call(
        final_kernel,
        out_shape=(shape((2, HALF, DIM)), shape((4, 12, DIM)), shape((48, DIM))),
        in_specs=vmem(5),
        out_specs=vmem(3),
        scratch_shapes=[pltpu.VMEM((4, 2, HALF, DIM), F32), pltpu.VMEM((4, HALF, DIM), F32), pltpu.VMEM((SPLIT, DIM), F32),
                        pltpu.VMEM((HALF - SPLIT, DIM), F32), pltpu.VMEM((2, HALF, DIM), F32), pltpu.VMEM((HALF, DIM), F32),
                        pltpu.VMEM((HALF, DIM), F32), pltpu.VMEM((4, 12, DIM), F32), pltpu.VMEM((4, 12, DIM), F32)]
        + plane_bufs() + plane_bufs() + [dma((2, 12)), dma((2, 12)), dma((2, 4)), dma((2, 6)), dma((2, 3)), dma((2,))],
        compiler_params=comm(4),
        cost_estimate=cost(2 * 4 * WIN * DIM * 4096, 20e6),
        name='final')(part, g_all, small_all, d_up, d_dn)


SWAP = [(0, 1), (1, 0)]


def step_program(token_rows, label_rows, table, up_block, down_block):
    me = lax.axis_index('stage')
    iz, iy, ix = lax.axis_index('z'), lax.axis_index('y'), lax.axis_index('x')
    own_up, own_dn = up_block[0], down_block[0]
    oth_up = lax.ppermute(own_up, 'stage', SWAP)
    oth_dn = lax.ppermute(own_dn, 'stage', SWAP)
    weights = (own_up, own_dn, oth_up, oth_dn)
    tok = lax.dynamic_index_in_dim(token_rows, me, 0, keepdims=False)
    lab = lax.dynamic_index_in_dim(label_rows, me, 0, keepdims=False)
    ids = jnp.concatenate([lab[None], lab[None]] + [tok[None]] * 6, axis=0).astype(F32)
    rows = table[jnp.concatenate([tok, lab])]
    x0, el = rows[:SEQ], rows[SEQ:]
    xs, x2, n, h = call_fwd(x0, *weights)
    n_all = lax.all_gather(n, ('y', 'x'), axis=0, tiled=True)
    gtop, small, ce, xg = call_head(n, lab[:, None], ids, el, x2, xs, table)
    go, g0, small_all = call_bwd(gtop, h, small, *weights)
    g_all = lax.all_gather(g0, ('y', 'x'), axis=0, tiled=True)
    part, gg = call_headgrad(table, n_all, small_all, go)
    d_up, d_dn = call_wgrad(xg, gg, own_up, own_dn)
    both, up_parts, grad_down = call_final(part, g_all, small_all, d_up, d_dn)
    grad_up = up_parts.transpose(1, 0, 2).reshape(1, 12, FFN)
    owner = (iz * 4 + iy) * 4 + ix
    begin = jnp.minimum(owner * ROWS // 16 * 16, VOCAB - WIN)
    grad_table = lax.dynamic_slice_in_dim(both.reshape(WIN, DIM), owner * ROWS - begin, ROWS, 0)
    losses = lax.all_gather(jnp.mean(ce).reshape(1), 'stage', axis=0, tiled=True)
    return losses, grad_table, grad_up, grad_down[None]


def solution(mesh):
    fine = jax.sharding.Mesh(mesh.devices.reshape(1, 4, 4, 4, 2), AXES)
    data = ('z', 'y', 'x')
    rows_spec = P(('pod',) + data, None)
    return jax.shard_map(step_program, mesh=fine,
                         in_specs=(rows_spec, rows_spec, P(None, None), P('stage', None, None), P('stage', None, None)),
                         out_specs=(P(('pod',) + data), rows_spec, P(('pod', 'stage'), data, None), P(('pod', 'stage'), data, None)),
                         check_vma=False)
```

```python
import itertools
import math

import jax
import jax.numpy as jnp
from jax import lax
from jax.experimental import pallas as pl
from jax.experimental.pallas import tpu as pltpu
from jax.sharding import PartitionSpec as P

NORM_EPS = 1e-6
BF = jnp.bfloat16
F32 = jnp.float32
VOCAB = 32128
DIM = 768
FFN = 3072
SEQ = 256
CHUNK = 768
NCH = FFN // CHUNK
ROWS = 502
WIN = 528
HALF = WIN // 2
SCALE = DIM ** -0.5
LOG2E = math.log2(math.e)
C2 = SCALE * LOG2E
GC = math.sqrt(2.0 / math.pi)
GA = 0.044715
VBLK = 4096
VSUB = 256
TBLK = 1024
VSTEPS = -(-VOCAB // VBLK)
HBLK = 512
HSTEPS = 16 * SEQ // HBLK
SPLIT = 136
URO = 12
DRO = 48
HSEQ = SEQ // 2
LANES = 128
SUBL = 8
LSE, LAB, TOK, CE = range(4)
ONE, OTHER = range(2)
SIDES = range(4)
AXES = ('pod', 'z', 'y', 'x', 'stage')

NT = (((1,), (1,)), ((), ()))
NN = (((1,), (0,)), ((), ()))
TN = (((0,), (0,)), ((), ()))


def dot(a, b, dims):
    return lax.dot_general(a, b, dims, preferred_element_type=F32)


def rows(fn, v):
    return fn(v, axis=-1, keepdims=True)


def cols(fn, v):
    return fn(v, axis=0, keepdims=True)


def inv_rms(wide):
    return lax.rsqrt(rows(jnp.mean, wide * wide) + NORM_EPS)


def column(row):
    return jnp.transpose(jnp.broadcast_to(row, (LANES, SEQ)))[:, :1]


def across(col):
    return jnp.transpose(jnp.broadcast_to(col, (SEQ, LANES)))[:SUBL]


def pair(sems, k):
    return sems.at[ONE, k], sems.at[OTHER, k]


def whole(dims):
    return pl.BlockSpec(dims, lambda i: (0,) * len(dims))


def gelu(h):
    return 0.5 * h * (1.0 + jnp.tanh(GC * (h + GA * h * h * h)))


def gelu_grad(h):
    t = jnp.tanh(GC * (h + GA * h * h * h))
    return 0.5 * (1.0 + t) + 0.5 * h * (1.0 - t * t) * (GC * (1.0 + 3.0 * GA * h * h))


def any_spec():
    return pl.BlockSpec(memory_space=pl.ANY)


def weight_copies(me, own_up, own_dn, oth_up, oth_dn, up_buf, dn_buf, sems):
    def up(ref, s, j):
        return pltpu.make_async_copy(ref.at[:, pl.ds(j * CHUNK, CHUNK)], up_buf.at[s, j], sems.at[s, j, 0])

    def dn(ref, s, j):
        return pltpu.make_async_copy(ref.at[pl.ds(j * CHUNK, CHUNK), :], dn_buf.at[s, j], sems.at[s, j, 1])

    def start(s, j):
        @pl.when(me == s)
        def _():
            up(own_up, s, j).start()
            dn(own_dn, s, j).start()

        @pl.when(me != s)
        def _():
            up(oth_up, s, j).start()
            dn(oth_dn, s, j).start()

    def wait(s, j):
        up(own_up, s, j).wait()
        dn(own_dn, s, j).wait()

    return start, wait


def fwd_kernel(x_ref, own_up, own_dn, oth_up, oth_dn, xs_ref, x2_ref, n_ref, h_ref, up_buf, dn_buf, sems):
    start, wait = weight_copies(lax.axis_index('stage'), own_up, own_dn, oth_up, oth_dn, up_buf, dn_buf, sems)
    for s in range(2):
        for j in range(NCH):
            start(s, j)
    x = x_ref[...]
    for s in range(2):
        xs_ref[s] = x
        acc = x.astype(F32)
        for j in range(NCH):
            wait(s, j)
            h = dot(x, up_buf[s, j], NN)
            h_ref[s, :, j * CHUNK:(j + 1) * CHUNK] = h
            acc = acc + dot(gelu(h).astype(BF), dn_buf[s, j], NN)
        x = acc.astype(BF)
    x2_ref[...] = x
    wide = x.astype(F32)
    inv = inv_rms(wide)
    n_ref[...] = (wide * inv).astype(BF)


def mod4(i):
    return lax.rem(i + 8, 4)


def ident(**kw):
    base = {name: lax.axis_index(name) for name in AXES}
    base.update(kw)
    return tuple(base[name] for name in AXES)


def remote(src, dst, send, recv, **kw):
    return pltpu.make_async_remote_copy(src_ref=src, dst_ref=dst, send_sem=send, recv_sem=recv, device_id=ident(**kw),
                                        device_id_type=pl.DeviceIdType.MESH)


def greet(targets):
    barrier = pltpu.get_barrier_semaphore()
    for kw in targets:
        pl.semaphore_signal(barrier, inc=1, device_id=ident(**kw), device_id_type=pl.DeviceIdType.MESH)
    pl.semaphore_wait(barrier, len(targets))


def bwd_kernel(g_ref, h_ref, small_ref, own_up, own_dn, oth_up, oth_dn, go_ref, g0_ref, all_ref, pair_ref,
               up_buf, dn_buf, sems, send, recv):
    me = lax.axis_index('stage')
    iy, ix = lax.axis_index('y'), lax.axis_index('x')
    start, wait = weight_copies(me, own_up, own_dn, oth_up, oth_dn, up_buf, dn_buf, sems)
    for s in (OTHER, ONE):
        for j in range(NCH):
            start(s, j)
    peers = [dict(y=mod4(iy + k // 4), x=mod4(ix + k % 4)) for k in range(1, 16)]
    targets = peers + [dict(stage=1 - me)]
    barrier = pltpu.get_barrier_semaphore()
    for kw in targets:
        pl.semaphore_signal(barrier, inc=1, device_id=ident(**kw), device_id_type=pl.DeviceIdType.MESH)
    copies = [remote(small_ref, pair_ref.at[me], send.at[ONE, 15], recv.at[ONE, 15], stage=1 - me)]
    for half, spot in enumerate(((iy, ix), (ix, iy))):
        copies += [remote(small_ref.at[half], all_ref.at[(half,) + spot], send.at[half, k], recv.at[half, k], **kw) for k, kw in enumerate(peers)]
    g = g_ref[...]
    for s in (1, 0):
        go_ref[s] = g
        acc = g.astype(F32)
        for j in range(NCH):
            wait(s, j)
            gg = dot(g, dn_buf[s, j], NT).astype(BF).astype(F32)
            gh = (gg * gelu_grad(h_ref[s, :, j * CHUNK:(j + 1) * CHUNK])).astype(BF)
            acc = acc + dot(gh, up_buf[s, j], NT)
        g = acc.astype(BF)
        if s == 1:
            pl.semaphore_wait(barrier, len(targets))
            for copy in copies:
                copy.start()
    g0_ref[...] = g
    all_ref[ONE, iy, ix] = small_ref[ONE]
    all_ref[OTHER, ix, iy] = small_ref[OTHER]
    pair_ref[me] = small_ref[...]
    for copy in copies:
        copy.wait()


class PlaneGather:
    def __init__(self, src, dst, local, send, recv):
        iy, ix = lax.axis_index('y'), lax.axis_index('x')
        yu, yd, xu, xd = mod4(iy + 1), mod4(iy - 1), mod4(ix + 1), mod4(ix - 1)
        self.targets = [dict(y=yu), dict(y=yd), dict(x=xu), dict(x=xd)]
        self.send, self.recv = send, recv
        self.own, self.phases = [], [[], [], [], []]
        parts = ((iy, ix, 'x', xu, xd, 'y', yu, yd), (ix, iy, 'y', yu, yd, 'x', xu, xd))
        for half, (a, b, near, bu, bd, wide, au, ad) in enumerate(parts):
            self.k = SUBL * half
            block = src.at[pl.ds(half * HSEQ, HSEQ), :]
            lo, hi = pl.ds(0, HSEQ // 2), pl.ds(HSEQ // 2, HSEQ // 2)
            out = dst.at[half]
            self.own.append(pltpu.make_async_copy(block, out.at[a, b], local.at[half]))
            left, right = out.at[ad, pl.ds(0, 2)], out.at[au, pl.ds(2, 2)]
            low, high = out.at[a, bd, lo], out.at[a, bu, hi]
            steps = ((block, out.at[a, b], block, near, bu, bd), (low, low, high, near, bu, bd),
                     (out.at[a], out.at[a], out.at[a], wide, au, ad), (left, left, right, wide, au, ad))
            for phase, (one, dst_one, two, name, upward, downward) in enumerate(steps):
                dst_two = out.at[a, b] if two is block else two
                self.phases[phase] += [self.copy(one, dst_one, name, upward), self.copy(two, dst_two, name, downward)]

    def copy(self, src, dst, name, target):
        self.k += 1
        return remote(src, dst, self.send.at[self.k - 1], self.recv.at[self.k - 1], **{name: target})

    def go(self, phase):
        if phase == 0:
            for copy in self.own:
                copy.start()
        else:
            for copy in self.phases[phase - 1]:
                copy.wait()
        if phase == 2:
            for copy in self.own:
                copy.wait()
        if phase < 4:
            for copy in self.phases[phase]:
                copy.start()


class ZGather:
    def __init__(self, src, dst, local, send, recv):
        me, iz = lax.axis_index('stage'), lax.axis_index('z')
        up, down = mod4(iz + 1), mod4(iz - 1)
        self.targets = [dict(stage=1 - me), dict(z=up), dict(z=down)]
        self.own = pltpu.make_async_copy(src.at[me], dst.at[iz, me], local)
        self.swap = remote(src.at[1 - me], dst.at[iz, me], send.at[4], recv.at[4], stage=1 - me)
        moves = ((dst.at[iz], dict(z=up)), (dst.at[iz], dict(z=down)), (dst.at[down, ONE], dict(z=up)), (dst.at[up, OTHER], dict(z=down)))
        moves = [remote(ref, ref, send.at[k], recv.at[k], **kw) for k, (ref, kw) in enumerate(moves)]
        self.first, self.second = moves[:2], moves[2:]

    def begin(self):
        self.swap.start()
        self.own.start()

    def spread(self):
        self.swap.wait()
        self.own.wait()
        for copy in self.first:
            copy.start()

    def forward(self):
        for copy in self.first:
            copy.wait()
        for copy in self.second:
            copy.start()

    def end(self):
        for copy in self.second:
            copy.wait()


def gather_hooks(step, plane, depth):
    @pl.when(step == 0)
    def _():
        greet(plane.targets + depth.targets)
        plane.go(0)
        depth.begin()

    @pl.when(step == 1)
    def _():
        plane.go(1)
        depth.spread()

    @pl.when(step == 2)
    def _():
        plane.go(2)

    @pl.when(step == 6)
    def _():
        plane.go(3)
        depth.forward()


def head_kernel(n_ref, lab_ref, ids_ref, el_ref, x2_ref, xs_ref, e_ref, gtop_ref, small_ref, nall_ref, xg_ref,
                acc_ref, m_ref, s_ref, pk_ref, local, send, recv, zlocal, zsend, zrecv):
    step = pl.program_id(0)
    plane = PlaneGather(n_ref, nall_ref, local, send, recv)
    depth = ZGather(xs_ref, xg_ref, zlocal, zsend, zrecv)
    gather_hooks(step, plane, depth)

    @pl.when(step == 0)
    def _():
        pk = across(rows(jnp.sum, n_ref[...].astype(F32) * el_ref[...].astype(F32)) * C2)
        pk_ref[...] = pk
        m_ref[...] = pk
        s_ref[...] = jnp.zeros_like(s_ref)
        acc_ref[...] = jnp.zeros_like(acc_ref)

    def run(count):
        n = n_ref[...]
        rel = lab_ref[...] - step * VBLK
        m = m_ref[:1, :]
        s = s_ref[:1, :]
        spans = [slice(lo, min(lo + VSUB, count)) for lo in range(0, count, VSUB)]
        ahead = dot(e_ref[spans[ONE], :], n, NT)
        for span, later in zip(spans, spans[1:] + [None]):
            l = ahead
            if later is not None:
                ahead = dot(e_ref[later, :], n, NT)
            new = jnp.maximum(m, cols(jnp.max, l) * C2)
            p = jnp.exp2(l * C2 - new)
            hit = lax.broadcasted_iota(jnp.int32, l.shape, 0) + span.start == rel
            p = jnp.where(hit, 0.0, p)
            alpha = jnp.exp2(m - new)
            s = s * alpha + cols(jnp.sum, p)
            acc_ref[...] = acc_ref[...] * alpha + dot(e_ref[span, :], p.astype(BF), TN)
            m = new
        m_ref[...] = jnp.broadcast_to(m, m_ref.shape)
        s_ref[...] = jnp.broadcast_to(s, s_ref.shape)

    @pl.when(step != VSTEPS - 1)
    def _():
        run(VBLK)

    @pl.when(step == VSTEPS - 1)
    def _():
        run(VOCAB % VBLK)
        m = m_ref[:1, :]
        s = s_ref[:1, :]
        pk = pk_ref[:1, :]
        total = s + jnp.exp2(pk - m)
        lse2 = m + jnp.log2(total)
        ce = (lse2 - pk) * (1.0 / LOG2E)
        row = lax.broadcasted_iota(jnp.int32, ids_ref.shape, 0)
        small = jnp.where(row == LSE, lse2, jnp.where(row == CE, ce, ids_ref[...]))
        small_ref[ONE] = small[:, :HSEQ]
        small_ref[OTHER] = small[:, HSEQ:]
        inv_total = 1.0 / total
        gn = jnp.transpose(acc_ref[...] * inv_total) - column(s * inv_total) * el_ref[...].astype(F32)
        gn = (gn * SCALE).astype(BF).astype(F32)
        wide = x2_ref[...].astype(F32)
        inv = inv_rms(wide)
        nw = wide * inv
        inner = rows(jnp.mean, gn * nw)
        gtop_ref[...] = (inv * (gn - nw * inner)).astype(BF)
        plane.go(4)
        depth.end()


def window_start(seg):
    owner = (seg * 4 + lax.axis_index('y')) * 4 + lax.axis_index('x')
    return jnp.minimum(owner * ROWS // 16 * 16, VOCAB - WIN)


def headgrad_kernel(table_ref, n_ref, all_ref, g0_ref, go_ref, out_ref, gall_ref, gg_ref, e_buf, sems,
                    local, send, recv, zlocal, zsend, zrecv):
    step = pl.program_id(0)
    plane = PlaneGather(g0_ref, gall_ref, local, send, recv)
    depth = ZGather(go_ref, gg_ref, zlocal, zsend, zrecv)

    def copy(seg):
        src = table_ref.at[pl.ds(pl.multiple_of(window_start(seg), 16), WIN), :]
        return pltpu.make_async_copy(src, e_buf.at[seg], sems.at[seg])

    @pl.when(step == 0)
    def _():
        for seg in SIDES:
            copy(seg).start()

    gather_hooks(step, plane, depth)

    @pl.when(step == 0)
    def _():
        out_ref[...] = jnp.zeros_like(out_ref)
        for seg in SIDES:
            copy(seg).wait()

    n = n_ref[...]
    def line(which):
        return jnp.concatenate([all_ref[ONE, ONE, q, pl.ds(which, 1), :] for q in SIDES], axis=1)

    lse = line(LSE) - math.log2(SCALE)
    lab = line(LAB).astype(jnp.int32)
    row = lax.broadcasted_iota(jnp.int32, (WIN, HBLK), 0)
    ahead = dot(e_buf[ONE], n, NT)
    for seg in SIDES:
        l = ahead
        if seg + 1 < len(SIDES):
            ahead = dot(e_buf[seg + 1], n, NT)
        p = jnp.exp2(l * C2 - lse)
        g = (p - jnp.where(row == lab - window_start(seg), SCALE, 0.0)).astype(BF)
        d = dot(g, n, NN)
        out_ref[seg, ONE] += d[:HALF]
        out_ref[seg, OTHER] += d[HALF:]

    @pl.when(step == HSTEPS - 1)
    def _():
        plane.go(4)
        depth.end()


def wgrad_kernel(*refs):
    x_refs, g_refs = refs[:4], refs[4:SUBL]
    up_ref, dn_ref, out_up, out_dn, wu, wd, acc_up, acc_dn, sems = refs[SUBL:]
    iz = lax.axis_index('z')
    first = pl.multiple_of(iz * CHUNK, CHUNK)
    cu = pltpu.make_async_copy(up_ref.at[:, pl.ds(first, CHUNK)], wu, sems.at[0])
    cd = pltpu.make_async_copy(dn_ref.at[pl.ds(first, CHUNK), :], wd, sems.at[1])
    cu.start()
    cd.start()
    cu.wait()
    cd.wait()
    for q in range(4):
        x = x_refs[q][ONE].reshape(2 * SEQ, DIM)
        g = g_refs[q][ONE].reshape(2 * SEQ, DIM)
        hid = dot(x, wu[...], NN)
        gg = dot(g, wd[...], NT).astype(BF).astype(F32)
        gated = gelu(hid).astype(BF)
        gh = (gg * gelu_grad(hid)).astype(BF)
        du = dot(x, gh, TN)
        dd = dot(gated, g, TN)
        acc_up[...] = acc_up[...] + du if q else du
        acc_dn[...] = acc_dn[...] + dd if q else dd
    for kz, ky, kx in itertools.product(SIDES, SIDES, SIDES):
        out_up[kx, ky, pl.ds(URO * kz, URO), :] = acc_up[pl.ds(URO * ((kz * 4 + ky) * 4 + kx), URO), :]
    for ky, kx in itertools.product(SIDES, SIDES):
        out_dn[ky, kx] = acc_dn[pl.ds(DRO * (ky * 4 + kx), DRO), :]


class PlaneReduce:
    def __init__(self, src, first, second, bufs, sems):
        self.src, self.bufs, self.sems = src, bufs, sems
        self.first, self.second = first, second

    def axis(self, name):
        i = lax.axis_index(name)
        return i, mod4(i + 1), mod4(i - 1), mod4(i + 2)

    def sem(self, k):
        return pair(self.sems, k)

    def pieces(self, phase):
        rel1, fin1, snd1, total, rel2, fin2, snd2 = self.bufs
        if phase == 0:
            name, src, rel, fin, snd, half, base = self.first, self.src, rel1, fin1, snd1, 2, 0
        else:
            name, src, rel, fin, snd, half, base = self.second, total, rel2, fin2, snd2, 24, 6
        i, up, down, far = self.axis(name)
        lo, hi = pl.ds(0, half), pl.ds(half, half)
        to_up, to_down = {name: up}, {name: down}
        moves = ((src.at[far, lo], rel.at[ONE], to_up), (src.at[far, hi], rel.at[OTHER], to_down),
                 (src.at[up, hi], fin.at[ONE, hi], to_up), (src.at[down, lo], fin.at[OTHER, lo], to_down),
                 (snd.at[ONE], fin.at[ONE, lo], to_up), (snd.at[OTHER], fin.at[OTHER, hi], to_down))
        moves = [remote(a, b, *self.sem(base + k), **kw) for k, (a, b, kw) in enumerate(moves)]
        early, late = moves[:4], moves[4:]
        return i, up, down, lo, hi, src, rel, fin, snd, early, late

    def start(self, phase):
        for copy in self.pieces(phase)[-2]:
            copy.start()

    def relay(self, phase):
        i, up, down, lo, hi, src, rel, fin, snd, early, late = self.pieces(phase)
        for side, part in enumerate((src.at[up, lo], src.at[down, hi])):
            early[side].wait_recv()
            snd[side] = part[...] + rel[side]
            late[side].start()

    def finish(self, phase):
        i, up, down, lo, hi, src, rel, fin, snd, early, late = self.pieces(phase)
        for copy in early[2:] + late:
            copy.wait_recv()
        return src[i] + fin[ONE] + fin[OTHER]

    def drain(self, phase):
        early, late = self.pieces(phase)[-2:]
        for copy in early + late:
            copy.wait_send()


def final_kernel(part_hbm, g_hbm, all_ref, up_ref, dn_ref, tab_ref, upo_ref, dno_ref,
                 part_ref, g_ref, lsems, t_ref, swap_ref, zrel0, zrel1, zfin, mine, theirs, u4, ugot, *rest):
    bufs_a, bufs_b, (sems_a, sems_b, sems_c, sems_z, sems_u, sems_f) = rest[:7], rest[7:14], rest[14:]
    me, iz, iy, ix = (lax.axis_index(name) for name in ('stage', 'z', 'y', 'x'))
    up, down, far = mod4(iz + 1), mod4(iz - 1), mod4(iz + 2)
    order = (far, up, down, iz)
    load = pltpu.make_async_copy(g_hbm, g_ref, lsems.at[4])
    pieces = [pltpu.make_async_copy(part_hbm.at[seg], part_ref.at[k], lsems.at[k]) for k, seg in enumerate(order)]
    for copy in [load] + pieces:
        copy.start()
    greet([dict(stage=1 - me), dict(z=up), dict(z=down), dict(z=far), dict(y=mod4(iy + 1)), dict(y=mod4(iy - 1)),
           dict(x=mod4(ix + 1)), dict(x=mod4(ix - 1))])
    red_a = PlaneReduce(up_ref, 'x', 'y', bufs_a, sems_a)
    red_b = PlaneReduce(dn_ref, 'y', 'x', bufs_b, sems_b)
    red_a.start(ONE)
    red_b.start(ONE)
    total_a, total_b = bufs_a[3], bufs_b[3]
    swaps = [remote(t_ref.at[seg, 1 - me], swap_ref.at[k], *pair(sems_c, k), stage=1 - me) for k, seg in enumerate(order)]
    lo, hi = pl.ds(0, SPLIT), pl.ds(SPLIT, HALF - SPLIT)

    to_up, to_down = dict(z=up), dict(z=down)
    moves = ((t_ref.at[far, me, lo], zrel0, to_up), (t_ref.at[far, me, hi], zrel1, to_down),
             (t_ref.at[up, me, hi], zfin.at[ONE, hi], to_up), (t_ref.at[up, me, lo], zfin.at[ONE, lo], to_up),
             (t_ref.at[down, me, lo], zfin.at[OTHER, lo], to_down), (t_ref.at[down, me, hi], zfin.at[OTHER, hi], to_down))
    moves = [remote(a, b, *pair(sems_z, k), **kw) for k, (a, b, kw) in enumerate(moves)]
    rel_up, rel_down, up_hi, up_lo, down_lo, down_hi = moves

    def embed(k):
        seg = order[k]
        row = lax.broadcasted_iota(jnp.int32, (WIN, TBLK), 0)
        pieces[k].wait()
        for b in SIDES:
            blocks = [divmod(SUBL * b + q, 4) for q in range(SUBL)]
            tok = jnp.concatenate([all_ref[i // 4, i % 4, q, pl.ds(TOK, 1), :] for i, q in blocks], axis=1).astype(jnp.int32)
            hot = jnp.where(row == tok - window_start(seg), 1.0, 0.0).astype(BF)
            d = dot(hot, g_ref[b * TBLK:(b + 1) * TBLK, :], NN)
            base = t_ref.at[seg] if b else part_ref.at[k]
            t_ref[seg, ONE] = base[ONE] + d[:HALF]
            t_ref[seg, OTHER] = base[OTHER] + d[HALF:]

    def merge(k):
        swaps[k].wait_recv()
        t_ref[order[k], me] += swap_ref[k]

    ifar, iup, idown, iown = SIDES
    load.wait()
    embed(ifar)
    swaps[ifar].start()
    embed(iup)
    merge(ifar)
    rel_up.start()
    rel_down.start()
    swaps[iup].start()
    red_a.relay(ONE)
    red_b.relay(ONE)
    embed(idown)
    merge(iup)
    up_hi.start()
    swaps[idown].start()
    embed(iown)
    merge(idown)
    down_lo.start()
    swaps[iown].start()
    rel_up.wait_recv()
    t_ref[up, me, lo] += zrel0[...]
    up_lo.start()
    rel_down.wait_recv()
    t_ref[down, me, hi] += zrel1[...]
    down_hi.start()
    total_a[...] = red_a.finish(ONE)
    red_a.start(OTHER)
    total_b[...] = red_b.finish(ONE)
    red_b.start(OTHER)
    swaps[iown].wait_recv()
    red_a.relay(OTHER)
    red_b.relay(OTHER)
    total = red_a.finish(OTHER)
    for k in SIDES:
        u4[k] = total[URO * k:URO * (k + 1), :]
    turns = [remote(u4.at[mod4(iz + k)], ugot.at[iz], *pair(sems_u, k), z=mod4(iz + k)) for k in SIDES[1:]]
    for copy in turns:
        copy.start()
    dno_ref[...] = red_b.finish(OTHER)
    for copy in (up_hi, up_lo, down_lo, down_hi):
        copy.wait_recv()
    mine[...] = t_ref[iz, me] + swap_ref[iown] + zfin[ONE] + zfin[OTHER]
    back = remote(mine, theirs, sems_f.at[ONE], sems_f.at[OTHER], stage=1 - me)
    back.start()
    tab_ref[me] = mine[...]
    for copy in turns:
        copy.wait_recv()
    upo_ref[...] = ugot[...]
    upo_ref[iz] = u4[iz]
    back.wait_recv()
    tab_ref[1 - me] = theirs[...]
    for copy in swaps + moves + [back] + turns:
        copy.wait_send()
    for phase in (ONE, OTHER):
        red_a.drain(phase)
        red_b.drain(phase)


def cost(flops, nbytes, trans=0):
    return pl.CostEstimate(flops=int(flops), bytes_accessed=int(nbytes), transcendentals=int(trans))


def vmem(n):
    return [pl.BlockSpec(memory_space=pltpu.VMEM)] * n


def shape(dims, dtype=F32):
    return jax.ShapeDtypeStruct(dims, dtype)


def comm(cid):
    return pltpu.CompilerParams(collective_id=cid, has_side_effects=True)


WBUFS = [pltpu.VMEM((2, NCH, DIM, CHUNK), BF), pltpu.VMEM((2, NCH, CHUNK, DIM), BF), pltpu.SemaphoreType.DMA((2, NCH, 2))]
GSEMS = [pltpu.SemaphoreType.DMA((2,)), pltpu.SemaphoreType.DMA((16,)), pltpu.SemaphoreType.DMA((16,)),
         pltpu.SemaphoreType.DMA, pltpu.SemaphoreType.DMA((5,)), pltpu.SemaphoreType.DMA((5,))]
PLANE = (2, 4, 4, SEQ // 2, DIM)
SMALL = (2, 4, 4, 8, SEQ // 2)


def call_fwd(x, *weights):
    tok = shape((SEQ, DIM), BF)
    return pl.pallas_call(
        fwd_kernel,
        out_shape=(shape((2, SEQ, DIM), BF), tok, tok, shape((2, SEQ, FFN))),
        in_specs=vmem(1) + [any_spec()] * 4,
        out_specs=vmem(4),
        scratch_shapes=WBUFS,
        cost_estimate=cost(8 * SEQ * DIM * FFN, 26e6),
        name='fwd')(x, *weights)


def call_bwd(g, h, small, *weights):
    return pl.pallas_call(
        bwd_kernel,
        out_shape=(shape((2, SEQ, DIM), BF), shape((SEQ, DIM), BF), shape(SMALL), shape((2, 2, 8, HSEQ))),
        in_specs=vmem(3) + [any_spec()] * 4,
        out_specs=vmem(4),
        scratch_shapes=WBUFS + [pltpu.SemaphoreType.DMA((2, 16)), pltpu.SemaphoreType.DMA((2, 16))],
        compiler_params=comm(1),
        cost_estimate=cost(8 * SEQ * DIM * FFN, 26e6),
        name='bwd')(g, h, small, *weights)


def call_head(n, lab, ids, el, x2, xs, table):
    return pl.pallas_call(
        head_kernel,
        grid=(VSTEPS,),
        out_shape=(shape((SEQ, DIM), BF), shape((2, 8, HSEQ)), shape(PLANE, BF), shape((4, 2, SEQ, DIM), BF)),
        in_specs=[whole((SEQ, DIM)), whole((1, SEQ)), whole((8, SEQ)), whole((SEQ, DIM)), whole((SEQ, DIM)), whole((2, SEQ, DIM)),
                  pl.BlockSpec((VBLK, DIM), lambda i: (i, 0))],
        out_specs=(whole((SEQ, DIM)), whole((2, 8, HSEQ)), any_spec(), any_spec()),
        scratch_shapes=[pltpu.VMEM((DIM, SEQ), F32)] + [pltpu.VMEM((8, SEQ), F32)] * 3 + GSEMS,
        compiler_params=comm(2),
        cost_estimate=cost(4 * SEQ * DIM * VOCAB, VOCAB * DIM * 2, SEQ * VOCAB),
        name='head')(n, lab, ids, el, x2, xs, table)


def call_headgrad(table, n_all, small_all, g0, go):
    toks = 16 * SEQ
    return pl.pallas_call(
        headgrad_kernel,
        grid=(HSTEPS,),
        out_shape=(shape((4, 2, HALF, DIM)), shape(PLANE, BF), shape((4, 2, SEQ, DIM), BF)),
        in_specs=[any_spec(), pl.BlockSpec((HBLK, DIM), lambda i: (i, 0)),
                  pl.BlockSpec((1, 1, 4, 8, HSEQ), lambda i: (i // 4, i % 4, 0, 0, 0)), whole((SEQ, DIM)), whole((2, SEQ, DIM))],
        out_specs=(whole((4, 2, HALF, DIM)), any_spec(), any_spec()),
        scratch_shapes=[pltpu.VMEM((4, WIN, DIM), BF), pltpu.SemaphoreType.DMA((4,))] + GSEMS,
        compiler_params=comm(3),
        cost_estimate=cost(4 * 4 * WIN * DIM * toks, 16e6, 4 * WIN * toks),
        name='headgrad')(table, n_all.reshape(toks, DIM), small_all, g0, go)


def call_wgrad(xg, gg, own_up, own_dn):
    block = lambda q: pl.BlockSpec((1, 2, SEQ, DIM), lambda i, q=q: (q, 0, 0, 0))
    res = whole((4, 4, DRO, DIM))
    return pl.pallas_call(
        wgrad_kernel,
        grid=(1,),
        out_shape=(shape((4, 4, DRO, DIM)), shape((4, 4, DRO, DIM))),
        in_specs=[block(q) for q in range(4)] * 2 + [any_spec()] * 2,
        out_specs=(res, res),
        scratch_shapes=[pltpu.VMEM((DIM, CHUNK), BF), pltpu.VMEM((CHUNK, DIM), BF), pltpu.VMEM((DIM, CHUNK), F32),
                        pltpu.VMEM((CHUNK, DIM), F32), pltpu.SemaphoreType.DMA((2,))],
        cost_estimate=cost(8 * 2048 * DIM * CHUNK, 16e6),
        name='wgrad')(*([xg] * 4), *([gg] * 4), own_up, own_dn)


def plane_bufs():
    return [pltpu.VMEM((2, 2, DRO, DIM), F32), pltpu.VMEM((2, 4, DRO, DIM), F32), pltpu.VMEM((2, 2, DRO, DIM), F32),
            pltpu.VMEM((4, DRO, DIM), F32), pltpu.VMEM((2, 24, DIM), F32), pltpu.VMEM((2, DRO, DIM), F32), pltpu.VMEM((2, 24, DIM), F32)]


def call_final(part, g_all, small_all, d_up, d_dn):
    dma = pltpu.SemaphoreType.DMA
    return pl.pallas_call(
        final_kernel,
        out_shape=(shape((2, HALF, DIM)), shape((4, URO, DIM)), shape((DRO, DIM))),
        in_specs=[any_spec()] * 2 + vmem(3),
        out_specs=vmem(3),
        scratch_shapes=[pltpu.VMEM((4, 2, HALF, DIM), F32), pltpu.VMEM((16 * SEQ, DIM), BF), dma((6,)), pltpu.VMEM((4, 2, HALF, DIM), F32), pltpu.VMEM((4, HALF, DIM), F32), pltpu.VMEM((SPLIT, DIM), F32),
                        pltpu.VMEM((HALF - SPLIT, DIM), F32), pltpu.VMEM((2, HALF, DIM), F32), pltpu.VMEM((HALF, DIM), F32),
                        pltpu.VMEM((HALF, DIM), F32), pltpu.VMEM((4, URO, DIM), F32), pltpu.VMEM((4, URO, DIM), F32)]
        + plane_bufs() + plane_bufs() + [dma((2, URO)), dma((2, URO)), dma((2, SUBL)), dma((2, SUBL)), dma((2, SUBL)), dma((2,))],
        compiler_params=comm(4),
        cost_estimate=cost(2 * 4 * WIN * DIM * 4096, 20e6),
        name='final')(part, g_all.reshape(16 * SEQ, DIM), small_all, d_up, d_dn)


SWAP = [(0, 1), (1, 0)]


def step_program(token_rows, label_rows, table, up_block, down_block):
    me = lax.axis_index('stage')
    iz, iy, ix = lax.axis_index('z'), lax.axis_index('y'), lax.axis_index('x')
    own_up, own_dn = up_block[0], down_block[0]
    oth_up = lax.ppermute(own_up, 'stage', SWAP)
    oth_dn = lax.ppermute(own_dn, 'stage', SWAP)
    weights = (own_up, own_dn, oth_up, oth_dn)
    tok = lax.dynamic_index_in_dim(token_rows, me, 0, keepdims=False)
    lab = lax.dynamic_index_in_dim(label_rows, me, 0, keepdims=False)
    ids = jnp.concatenate([lab[None], lab[None]] + [tok[None]] * 6, axis=0).astype(F32)
    rows = table[jnp.concatenate([tok, lab])]
    x0, el = rows[:SEQ], rows[SEQ:]
    xs, x2, n, h = call_fwd(x0, *weights)
    gtop, small, n_all, xg = call_head(n, lab[None], ids, el, x2, xs, table)
    go, g0, small_all, pair = call_bwd(gtop, h, small, *weights)
    part, g_all, gg = call_headgrad(table, n_all, small_all, g0, go)
    d_up, d_dn = call_wgrad(xg, gg, own_up, own_dn)
    both, up_parts, grad_down = call_final(part, g_all, small_all, d_up, d_dn)
    grad_up = up_parts.transpose(1, 0, 2).reshape(1, URO, FFN)
    owner = (iz * 4 + iy) * 4 + ix
    begin = jnp.minimum(owner * ROWS // 16 * 16, VOCAB - WIN)
    grad_table = lax.dynamic_slice_in_dim(both.reshape(WIN, DIM), owner * ROWS - begin, ROWS, 0)
    losses = jnp.mean(pair[:, :, 3, :], axis=(1, 2))
    return losses, grad_table, grad_up, grad_down[None]


def solution(mesh):
    fine = jax.sharding.Mesh(mesh.devices.reshape(1, 4, 4, 4, 2), AXES)
    data = ('z', 'y', 'x')
    rows_spec = P(('pod',) + data, None)
    return jax.shard_map(step_program, mesh=fine,
                         in_specs=(rows_spec, rows_spec, P(None, None), P('stage', None, None), P('stage', None, None)),
                         out_specs=(P(('pod',) + data), rows_spec, P(('pod', 'stage'), data, None), P(('pod', 'stage'), data, None)),
                         check_vma=False)
```

```python
import itertools
import math

import jax
import jax.numpy as jnp
from jax import lax
from jax.experimental import pallas as pl
from jax.experimental.pallas import tpu as pltpu
from jax.sharding import PartitionSpec as P

NORM_EPS = 1e-6
BF = jnp.bfloat16
F32 = jnp.float32
VOCAB = 32128
DIM = 768
FFN = 3072
SEQ = 256
CHUNK = 768
NCH = FFN // CHUNK
ROWS = 502
WIN = 528
HALF = WIN // 2
SCALE = DIM ** -0.5
LOG2E = math.log2(math.e)
C2 = SCALE * LOG2E
GC = math.sqrt(2.0 / math.pi)
GA = 0.044715
VBLK = 4096
VSUB = 256
TBLK = 1024
VSTEPS = -(-VOCAB // VBLK)
HBLK = 512
HSTEPS = 16 * SEQ // HBLK
SPLIT = 136
URO = 12
DRO = 48
HSEQ = SEQ // 2
LANES = 128
SUBL = 8
LSE, LAB, TOK, CE = range(4)
ONE, OTHER = range(2)
SIDES = range(4)
AXES = ('pod', 'z', 'y', 'x', 'stage')

NT = (((1,), (1,)), ((), ()))
NN = (((1,), (0,)), ((), ()))
TN = (((0,), (0,)), ((), ()))


def dot(a, b, dims):
    return lax.dot_general(a, b, dims, preferred_element_type=F32)


def rows(fn, v):
    return fn(v, axis=-1, keepdims=True)


def cols(fn, v):
    return fn(v, axis=0, keepdims=True)


def inv_rms(wide):
    return lax.rsqrt(rows(jnp.mean, wide * wide) + NORM_EPS)


def column(row):
    return jnp.transpose(jnp.broadcast_to(row, (LANES, SEQ)))[:, :1]


def across(col):
    return jnp.transpose(jnp.broadcast_to(col, (SEQ, LANES)))[:SUBL]


def pair(sems, k):
    return sems.at[ONE, k], sems.at[OTHER, k]


def whole(dims):
    return pl.BlockSpec(dims, lambda i: (0,) * len(dims))


def gelu(h):
    return 0.5 * h * (1.0 + jnp.tanh(GC * (h + GA * h * h * h)))


def gelu_grad(h):
    t = jnp.tanh(GC * (h + GA * h * h * h))
    return 0.5 * (1.0 + t) + 0.5 * h * (1.0 - t * t) * (GC * (1.0 + 3.0 * GA * h * h))


def any_spec():
    return pl.BlockSpec(memory_space=pl.ANY)


def weight_copies(me, own_up, own_dn, oth_up, oth_dn, up_buf, dn_buf, sems):
    def up(ref, s, j):
        return pltpu.make_async_copy(ref.at[:, pl.ds(j * CHUNK, CHUNK)], up_buf.at[s, j], sems.at[s, j, 0])

    def dn(ref, s, j):
        return pltpu.make_async_copy(ref.at[pl.ds(j * CHUNK, CHUNK), :], dn_buf.at[s, j], sems.at[s, j, 1])

    def start(s, j):
        @pl.when(me == s)
        def _():
            up(own_up, s, j).start()
            dn(own_dn, s, j).start()

        @pl.when(me != s)
        def _():
            up(oth_up, s, j).start()
            dn(oth_dn, s, j).start()

    def wait(s, j):
        up(own_up, s, j).wait()
        dn(own_dn, s, j).wait()

    return start, wait


def fwd_kernel(x_ref, own_up, own_dn, oth_up, oth_dn, xs_ref, x2_ref, n_ref, h_hbm, up_buf, dn_buf, sems, h_ref, hsems):
    start, wait = weight_copies(lax.axis_index('stage'), own_up, own_dn, oth_up, oth_dn, up_buf, dn_buf, sems)
    for s in range(2):
        for j in range(NCH):
            start(s, j)
    x = x_ref[...]
    kept = []
    for s in range(2):
        xs_ref[s] = x
        acc = x.astype(F32)
        for j in range(NCH):
            wait(s, j)
            h = dot(x, up_buf[s, j], NN)
            h_ref[s, j] = h
            keep = pltpu.make_async_copy(h_ref.at[s, j], h_hbm.at[s, j], hsems.at[s, j])
            keep.start()
            kept.append(keep)
            acc = acc + dot(gelu(h).astype(BF), dn_buf[s, j], NN)
        x = acc.astype(BF)
    x2_ref[...] = x
    wide = x.astype(F32)
    inv = inv_rms(wide)
    n_ref[...] = (wide * inv).astype(BF)
    for keep in kept:
        keep.wait()


def mod4(i):
    return lax.rem(i + 8, 4)


def ident(**kw):
    base = {name: lax.axis_index(name) for name in AXES}
    base.update(kw)
    return tuple(base[name] for name in AXES)


def remote(src, dst, send, recv, **kw):
    return pltpu.make_async_remote_copy(src_ref=src, dst_ref=dst, send_sem=send, recv_sem=recv, device_id=ident(**kw),
                                        device_id_type=pl.DeviceIdType.MESH)


def greet(targets):
    barrier = pltpu.get_barrier_semaphore()
    for kw in targets:
        pl.semaphore_signal(barrier, inc=1, device_id=ident(**kw), device_id_type=pl.DeviceIdType.MESH)
    pl.semaphore_wait(barrier, len(targets))


def bwd_kernel(g_ref, h_hbm, small_ref, own_up, own_dn, oth_up, oth_dn, go_ref, g0_ref, all_ref, pair_ref,
               up_buf, dn_buf, sems, h_ref, hsems, send, recv):
    me = lax.axis_index('stage')
    iy, ix = lax.axis_index('y'), lax.axis_index('x')
    start, wait = weight_copies(me, own_up, own_dn, oth_up, oth_dn, up_buf, dn_buf, sems)
    def take(s, j):
        return pltpu.make_async_copy(h_hbm.at[s, j], h_ref.at[s, j], hsems.at[s, j])

    for s in (OTHER, ONE):
        for j in range(NCH):
            start(s, j)
            take(s, j).start()
    peers = [dict(y=mod4(iy + k // 4), x=mod4(ix + k % 4)) for k in range(1, 16)]
    targets = peers + [dict(stage=1 - me)]
    barrier = pltpu.get_barrier_semaphore()
    for kw in targets:
        pl.semaphore_signal(barrier, inc=1, device_id=ident(**kw), device_id_type=pl.DeviceIdType.MESH)
    copies = [remote(small_ref, pair_ref.at[me], send.at[ONE, 15], recv.at[ONE, 15], stage=1 - me)]
    for half, spot in enumerate(((iy, ix), (ix, iy))):
        copies += [remote(small_ref.at[half], all_ref.at[(half,) + spot], send.at[half, k], recv.at[half, k], **kw) for k, kw in enumerate(peers)]
    g = g_ref[...]
    for s in (1, 0):
        go_ref[s] = g
        acc = g.astype(F32)
        for j in range(NCH):
            wait(s, j)
            gg = dot(g, dn_buf[s, j], NT).astype(BF).astype(F32)
            take(s, j).wait()
            gh = (gg * gelu_grad(h_ref[s, j])).astype(BF)
            acc = acc + dot(gh, up_buf[s, j], NT)
        g = acc.astype(BF)
        if s == 1:
            pl.semaphore_wait(barrier, len(targets))
            for copy in copies:
                copy.start()
    g0_ref[...] = g
    all_ref[ONE, iy, ix] = small_ref[ONE]
    all_ref[OTHER, ix, iy] = small_ref[OTHER]
    pair_ref[me] = small_ref[...]
    for copy in copies:
        copy.wait()


class PlaneGather:
    def __init__(self, src, dst, local, send, recv):
        iy, ix = lax.axis_index('y'), lax.axis_index('x')
        yu, yd, xu, xd = mod4(iy + 1), mod4(iy - 1), mod4(ix + 1), mod4(ix - 1)
        self.targets = [dict(y=yu), dict(y=yd), dict(x=xu), dict(x=xd)]
        self.send, self.recv = send, recv
        self.own, self.phases = [], [[] for _ in range(6)]
        parts = ((iy, ix, 'x', xu, xd, 'y', yu, yd), (ix, iy, 'y', yu, yd, 'x', xu, xd))
        for half, (a, b, near, bu, bd, wide, au, ad) in enumerate(parts):
            self.k = 16 * half
            block = src.at[pl.ds(half * HSEQ, HSEQ), :]
            lo, hi = pl.ds(0, HSEQ // 2), pl.ds(HSEQ // 2, HSEQ // 2)
            out = dst.at[half]
            self.own.append(pltpu.make_async_copy(block, out.at[a, b], local.at[half]))
            left, right = out.at[ad, pl.ds(0, 2)], out.at[au, pl.ds(2, 2)]
            low, high = out.at[a, bd, lo], out.at[a, bu, hi]
            far = mod4(b + 2)
            steps = ((ONE, block, out.at[a, b], block, near, bu, bd), (OTHER, low, low, high, near, bu, bd),
                     (4, block, out.at[a, b], block, wide, au, ad), (5, out.at[a, bd], out.at[a, bd], out.at[a, bd], wide, au, ad),
                     (5, out.at[a, bu], out.at[a, bu], out.at[a, bu], wide, au, ad),
                     (2, out.at[a, far], out.at[a, far], out.at[a, far], wide, au, ad), (3, left, left, right, wide, au, ad))
            for phase, one, dst_one, two, name, upward, downward in steps:
                dst_two = out.at[a, b] if two is block else two
                self.phases[phase] += [self.copy(one, dst_one, name, upward), self.copy(two, dst_two, name, downward)]

    def copy(self, src, dst, name, target):
        self.k += 1
        return remote(src, dst, self.send.at[self.k - 1], self.recv.at[self.k - 1], **{name: target})

    def go(self, phase):
        near, relay, far, last, own, sides = self.phases
        starts = (self.own + near + own, relay + sides, far, last, [])
        waits = ([], near + self.own, relay, own + sides + far, last)
        for copy in waits[phase]:
            copy.wait()
        for copy in starts[phase]:
            copy.start()


class ZGather:
    def __init__(self, src, dst, local, send, recv):
        me, iz = lax.axis_index('stage'), lax.axis_index('z')
        up, down = mod4(iz + 1), mod4(iz - 1)
        self.targets = [dict(stage=1 - me), dict(z=up), dict(z=down)]
        self.own = pltpu.make_async_copy(src.at[me], dst.at[iz, me], local)
        self.swap = remote(src.at[1 - me], dst.at[iz, me], send.at[4], recv.at[4], stage=1 - me)
        moves = ((dst.at[iz], dict(z=up)), (dst.at[iz], dict(z=down)), (dst.at[down, ONE], dict(z=up)), (dst.at[up, OTHER], dict(z=down)))
        moves = [remote(ref, ref, send.at[k], recv.at[k], **kw) for k, (ref, kw) in enumerate(moves)]
        self.first, self.second = moves[:2], moves[2:]

    def begin(self):
        self.swap.start()
        self.own.start()

    def spread(self):
        self.swap.wait()
        self.own.wait()
        for copy in self.first:
            copy.start()

    def forward(self):
        for copy in self.first:
            copy.wait()
        for copy in self.second:
            copy.start()

    def end(self):
        for copy in self.second:
            copy.wait()


def gather_hooks(step, plane, depth):
    @pl.when(step == 0)
    def _():
        greet(plane.targets + depth.targets)
        plane.go(0)
        depth.begin()

    @pl.when(step == 1)
    def _():
        plane.go(1)
        depth.spread()

    @pl.when(step == 3)
    def _():
        plane.go(2)

    @pl.when(step == 6)
    def _():
        plane.go(3)
        depth.forward()


def head_kernel(n_ref, lab_ref, ids_ref, el_ref, x2_ref, xs_ref, e_ref, gtop_ref, small_ref, nall_ref, xg_ref,
                acc_ref, m_ref, s_ref, pk_ref, local, send, recv, zlocal, zsend, zrecv):
    step = pl.program_id(0)
    plane = PlaneGather(n_ref, nall_ref, local, send, recv)
    depth = ZGather(xs_ref, xg_ref, zlocal, zsend, zrecv)
    gather_hooks(step, plane, depth)

    @pl.when(step == 0)
    def _():
        pk = across(rows(jnp.sum, n_ref[...].astype(F32) * el_ref[...].astype(F32)) * C2)
        pk_ref[...] = pk
        m_ref[...] = pk
        s_ref[...] = jnp.zeros_like(s_ref)
        acc_ref[...] = jnp.zeros_like(acc_ref)

    def run(count):
        n = n_ref[...]
        rel = lab_ref[...] - step * VBLK
        m = m_ref[:1, :]
        s = s_ref[:1, :]
        spans = [slice(lo, min(lo + VSUB, count)) for lo in range(0, count, VSUB)]
        ahead = dot(e_ref[spans[ONE], :], n, NT)
        for span, later in zip(spans, spans[1:] + [None]):
            l = ahead
            if later is not None:
                ahead = dot(e_ref[later, :], n, NT)
            new = jnp.maximum(m, cols(jnp.max, l) * C2)
            p = jnp.exp2(l * C2 - new)
            hit = lax.broadcasted_iota(jnp.int32, l.shape, 0) + span.start == rel
            p = jnp.where(hit, 0.0, p)
            alpha = jnp.exp2(m - new)
            s = s * alpha + cols(jnp.sum, p)
            acc_ref[...] = acc_ref[...] * alpha + dot(e_ref[span, :], p.astype(BF), TN)
            m = new
        m_ref[...] = jnp.broadcast_to(m, m_ref.shape)
        s_ref[...] = jnp.broadcast_to(s, s_ref.shape)

    @pl.when(step != VSTEPS - 1)
    def _():
        run(VBLK)

    @pl.when(step == VSTEPS - 1)
    def _():
        run(VOCAB % VBLK)
        m = m_ref[:1, :]
        s = s_ref[:1, :]
        pk = pk_ref[:1, :]
        total = s + jnp.exp2(pk - m)
        lse2 = m + jnp.log2(total)
        ce = (lse2 - pk) * (1.0 / LOG2E)
        row = lax.broadcasted_iota(jnp.int32, ids_ref.shape, 0)
        small = jnp.where(row == LSE, lse2, jnp.where(row == CE, ce, ids_ref[...]))
        small_ref[ONE] = small[:, :HSEQ]
        small_ref[OTHER] = small[:, HSEQ:]
        inv_total = 1.0 / total
        gn = jnp.transpose(acc_ref[...] * inv_total) - column(s * inv_total) * el_ref[...].astype(F32)
        gn = (gn * SCALE).astype(BF).astype(F32)
        wide = x2_ref[...].astype(F32)
        inv = inv_rms(wide)
        nw = wide * inv
        inner = rows(jnp.mean, gn * nw)
        gtop_ref[...] = (inv * (gn - nw * inner)).astype(BF)
        plane.go(4)
        depth.end()


def window_start(seg):
    owner = (seg * 4 + lax.axis_index('y')) * 4 + lax.axis_index('x')
    return jnp.minimum(owner * ROWS // 16 * 16, VOCAB - WIN)


def headgrad_kernel(table_ref, n_ref, all_ref, g0_ref, go_ref, out_ref, gall_ref, gg_ref, e_buf, sems,
                    local, send, recv, zlocal, zsend, zrecv):
    step = pl.program_id(0)
    plane = PlaneGather(g0_ref, gall_ref, local, send, recv)
    depth = ZGather(go_ref, gg_ref, zlocal, zsend, zrecv)

    def copy(seg):
        src = table_ref.at[pl.ds(pl.multiple_of(window_start(seg), 16), WIN), :]
        return pltpu.make_async_copy(src, e_buf.at[seg], sems.at[seg])

    @pl.when(step == 0)
    def _():
        for seg in SIDES:
            copy(seg).start()

    gather_hooks(step, plane, depth)

    @pl.when(step == 0)
    def _():
        out_ref[...] = jnp.zeros_like(out_ref)
        for seg in SIDES:
            copy(seg).wait()

    n = n_ref[...]
    def line(which):
        return jnp.concatenate([all_ref[ONE, ONE, q, pl.ds(which, 1), :] for q in SIDES], axis=1)

    lse = line(LSE) - math.log2(SCALE)
    lab = line(LAB).astype(jnp.int32)
    row = lax.broadcasted_iota(jnp.int32, (WIN, HBLK), 0)
    ahead = dot(e_buf[ONE], n, NT)
    for seg in SIDES:
        l = ahead
        if seg + 1 < len(SIDES):
            ahead = dot(e_buf[seg + 1], n, NT)
        p = jnp.exp2(l * C2 - lse)
        g = (p - jnp.where(row == lab - window_start(seg), SCALE, 0.0)).astype(BF)
        d = dot(g, n, NN)
        out_ref[seg, ONE] += d[:HALF]
        out_ref[seg, OTHER] += d[HALF:]

    @pl.when(step == HSTEPS - 1)
    def _():
        plane.go(4)
        depth.end()


def wgrad_kernel(xg_ref, gg_ref, up_ref, dn_ref, out_up, out_dn, wu, wd, acc_up, acc_dn, xbuf, gbuf, sems, xsems, gsems):
    iz = lax.axis_index('z')
    first = pl.multiple_of(iz * CHUNK, CHUNK)
    cu = pltpu.make_async_copy(up_ref.at[:, pl.ds(first, CHUNK)], wu, sems.at[ONE])
    cd = pltpu.make_async_copy(dn_ref.at[pl.ds(first, CHUNK), :], wd, sems.at[OTHER])
    loads = [(pltpu.make_async_copy(xg_ref.at[q], xbuf.at[q], xsems.at[q]), pltpu.make_async_copy(gg_ref.at[q], gbuf.at[q], gsems.at[q])) for q in SIDES]
    cu.start()
    for some in loads:
        for copy in some:
            copy.start()
        if some is loads[ONE]:
            cd.start()
    cu.wait()
    for q in SIDES:
        for copy in loads[q]:
            copy.wait()
        if q == ONE:
            cd.wait()
        x = xbuf[q].reshape(2 * SEQ, DIM)
        g = gbuf[q].reshape(2 * SEQ, DIM)
        hid = dot(x, wu[...], NN)
        gg = dot(g, wd[...], NT).astype(BF).astype(F32)
        gated = gelu(hid).astype(BF)
        gh = (gg * gelu_grad(hid)).astype(BF)
        du = dot(x, gh, TN)
        dd = dot(gated, g, TN)
        acc_up[...] = acc_up[...] + du if q else du
        acc_dn[...] = acc_dn[...] + dd if q else dd
    for kz, ky, kx in itertools.product(SIDES, SIDES, SIDES):
        out_up[kx, ky, pl.ds(URO * kz, URO), :] = acc_up[pl.ds(URO * ((kz * 4 + ky) * 4 + kx), URO), :]
    for ky, kx in itertools.product(SIDES, SIDES):
        out_dn[ky, kx] = acc_dn[pl.ds(DRO * (ky * 4 + kx), DRO), :]


class PlaneReduce:
    def __init__(self, src, first, second, bufs, sems):
        self.src, self.bufs, self.sems = src, bufs, sems
        self.first, self.second = first, second

    def axis(self, name):
        i = lax.axis_index(name)
        return i, mod4(i + 1), mod4(i - 1), mod4(i + 2)

    def sem(self, k):
        return pair(self.sems, k)

    def pieces(self, phase):
        rel1, fin1, snd1, total, rel2, fin2, snd2 = self.bufs
        if phase == 0:
            name, src, rel, fin, snd, half, base = self.first, self.src, rel1, fin1, snd1, 2, 0
        else:
            name, src, rel, fin, snd, half, base = self.second, total, rel2, fin2, snd2, 24, 6
        i, up, down, far = self.axis(name)
        lo, hi = pl.ds(0, half), pl.ds(half, half)
        to_up, to_down = {name: up}, {name: down}
        moves = ((src.at[far, lo], rel.at[ONE], to_up), (src.at[far, hi], rel.at[OTHER], to_down),
                 (src.at[up, hi], fin.at[ONE, hi], to_up), (src.at[down, lo], fin.at[OTHER, lo], to_down),
                 (snd.at[ONE], fin.at[ONE, lo], to_up), (snd.at[OTHER], fin.at[OTHER, hi], to_down))
        moves = [remote(a, b, *self.sem(base + k), **kw) for k, (a, b, kw) in enumerate(moves)]
        early, late = moves[:4], moves[4:]
        return i, up, down, lo, hi, src, rel, fin, snd, early, late

    def start(self, phase):
        for copy in self.pieces(phase)[-2]:
            copy.start()

    def relay(self, phase):
        i, up, down, lo, hi, src, rel, fin, snd, early, late = self.pieces(phase)
        for side, part in enumerate((src.at[up, lo], src.at[down, hi])):
            early[side].wait_recv()
            snd[side] = part[...] + rel[side]
            late[side].start()

    def finish(self, phase):
        i, up, down, lo, hi, src, rel, fin, snd, early, late = self.pieces(phase)
        for copy in early[2:] + late:
            copy.wait_recv()
        return src[i] + fin[ONE] + fin[OTHER]

    def drain(self, phase):
        early, late = self.pieces(phase)[-2:]
        for copy in early + late:
            copy.wait_send()


def final_kernel(part_hbm, g_hbm, all_ref, up_ref, dn_ref, tab_ref, upo_ref, dno_ref,
                 part_ref, g_ref, lsems, t_ref, swap_ref, zrel0, zrel1, zfin, mine, theirs, u4, ugot, *rest):
    bufs_a, bufs_b, (sems_a, sems_b, sems_c, sems_z, sems_u, sems_f) = rest[:7], rest[7:14], rest[14:]
    me, iz, iy, ix = (lax.axis_index(name) for name in ('stage', 'z', 'y', 'x'))
    up, down, far = mod4(iz + 1), mod4(iz - 1), mod4(iz + 2)
    order = (far, up, down, iz)
    load = pltpu.make_async_copy(g_hbm, g_ref, lsems.at[4])
    pieces = [pltpu.make_async_copy(part_hbm.at[seg], part_ref.at[k], lsems.at[k]) for k, seg in enumerate(order)]
    for copy in [load] + pieces:
        copy.start()
    greet([dict(stage=1 - me), dict(z=up), dict(z=down), dict(z=far), dict(y=mod4(iy + 1)), dict(y=mod4(iy - 1)),
           dict(x=mod4(ix + 1)), dict(x=mod4(ix - 1))])
    red_a = PlaneReduce(up_ref, 'x', 'y', bufs_a, sems_a)
    red_b = PlaneReduce(dn_ref, 'y', 'x', bufs_b, sems_b)
    red_a.start(ONE)
    red_b.start(ONE)
    total_a, total_b = bufs_a[3], bufs_b[3]
    swaps = [remote(t_ref.at[seg, 1 - me], swap_ref.at[k], *pair(sems_c, k), stage=1 - me) for k, seg in enumerate(order)]
    lo, hi = pl.ds(0, SPLIT), pl.ds(SPLIT, HALF - SPLIT)

    to_up, to_down = dict(z=up), dict(z=down)
    moves = ((t_ref.at[far, me, lo], zrel0, to_up), (t_ref.at[far, me, hi], zrel1, to_down),
             (t_ref.at[up, me, hi], zfin.at[ONE, hi], to_up), (t_ref.at[up, me, lo], zfin.at[ONE, lo], to_up),
             (t_ref.at[down, me, lo], zfin.at[OTHER, lo], to_down), (t_ref.at[down, me, hi], zfin.at[OTHER, hi], to_down))
    moves = [remote(a, b, *pair(sems_z, k), **kw) for k, (a, b, kw) in enumerate(moves)]
    rel_up, rel_down, up_hi, up_lo, down_lo, down_hi = moves

    def embed(k):
        seg = order[k]
        row = lax.broadcasted_iota(jnp.int32, (WIN, TBLK), 0)
        pieces[k].wait()
        for b in SIDES:
            blocks = [divmod(SUBL * b + q, 4) for q in range(SUBL)]
            tok = jnp.concatenate([all_ref[i // 4, i % 4, q, pl.ds(TOK, 1), :] for i, q in blocks], axis=1).astype(jnp.int32)
            hot = jnp.where(row == tok - window_start(seg), 1.0, 0.0).astype(BF)
            d = dot(hot, g_ref[b * TBLK:(b + 1) * TBLK, :], NN)
            base = t_ref.at[seg] if b else part_ref.at[k]
            t_ref[seg, ONE] = base[ONE] + d[:HALF]
            t_ref[seg, OTHER] = base[OTHER] + d[HALF:]

    def merge(k):
        swaps[k].wait_recv()
        t_ref[order[k], me] += swap_ref[k]

    ifar, iup, idown, iown = SIDES
    load.wait()
    embed(ifar)
    swaps[ifar].start()
    embed(iup)
    merge(ifar)
    rel_up.start()
    rel_down.start()
    swaps[iup].start()
    red_a.relay(ONE)
    red_b.relay(ONE)
    embed(idown)
    merge(iup)
    up_hi.start()
    swaps[idown].start()
    embed(iown)
    merge(idown)
    down_lo.start()
    swaps[iown].start()
    rel_up.wait_recv()
    t_ref[up, me, lo] += zrel0[...]
    up_lo.start()
    rel_down.wait_recv()
    t_ref[down, me, hi] += zrel1[...]
    down_hi.start()
    total_a[...] = red_a.finish(ONE)
    red_a.start(OTHER)
    total_b[...] = red_b.finish(ONE)
    red_b.start(OTHER)
    swaps[iown].wait_recv()
    red_a.relay(OTHER)
    red_b.relay(OTHER)
    total = red_a.finish(OTHER)
    for k in SIDES:
        u4[k] = total[URO * k:URO * (k + 1), :]
    turns = [remote(u4.at[mod4(iz + k)], ugot.at[iz], *pair(sems_u, k), z=mod4(iz + k)) for k in SIDES[1:]]
    for copy in turns:
        copy.start()
    dno_ref[...] = red_b.finish(OTHER)
    for copy in (up_hi, up_lo, down_lo, down_hi):
        copy.wait_recv()
    mine[...] = t_ref[iz, me] + swap_ref[iown] + zfin[ONE] + zfin[OTHER]
    back = remote(mine, theirs, sems_f.at[ONE], sems_f.at[OTHER], stage=1 - me)
    back.start()
    tab_ref[me] = mine[...]
    for copy in turns:
        copy.wait_recv()
    upo_ref[...] = ugot[...]
    upo_ref[iz] = u4[iz]
    back.wait_recv()
    tab_ref[1 - me] = theirs[...]
    for copy in swaps + moves + [back] + turns:
        copy.wait_send()
    for phase in (ONE, OTHER):
        red_a.drain(phase)
        red_b.drain(phase)


def cost(flops, nbytes, trans=0):
    return pl.CostEstimate(flops=int(flops), bytes_accessed=int(nbytes), transcendentals=int(trans))


def vmem(n):
    return [pl.BlockSpec(memory_space=pltpu.VMEM)] * n


def shape(dims, dtype=F32):
    return jax.ShapeDtypeStruct(dims, dtype)


def comm(cid):
    return pltpu.CompilerParams(collective_id=cid, has_side_effects=True)


WBUFS = [pltpu.VMEM((2, NCH, DIM, CHUNK), BF), pltpu.VMEM((2, NCH, CHUNK, DIM), BF), pltpu.SemaphoreType.DMA((2, NCH, 2)),
         pltpu.VMEM((2, NCH, SEQ, CHUNK), F32), pltpu.SemaphoreType.DMA((2, NCH))]
HID = (2, NCH, SEQ, CHUNK)
GSEMS = [pltpu.SemaphoreType.DMA((2,)), pltpu.SemaphoreType.DMA((32,)), pltpu.SemaphoreType.DMA((32,)),
         pltpu.SemaphoreType.DMA, pltpu.SemaphoreType.DMA((5,)), pltpu.SemaphoreType.DMA((5,))]
PLANE = (2, 4, 4, SEQ // 2, DIM)
SMALL = (2, 4, 4, 8, SEQ // 2)


def call_fwd(x, *weights):
    tok = shape((SEQ, DIM), BF)
    return pl.pallas_call(
        fwd_kernel,
        out_shape=(shape((2, SEQ, DIM), BF), tok, tok, shape(HID)),
        in_specs=vmem(1) + [any_spec()] * 4,
        out_specs=vmem(3) + [any_spec()],
        scratch_shapes=WBUFS,
        cost_estimate=cost(8 * SEQ * DIM * FFN, 26e6),
        name='fwd')(x, *weights)


def call_bwd(g, h, small, *weights):
    return pl.pallas_call(
        bwd_kernel,
        out_shape=(shape((2, SEQ, DIM), BF), shape((SEQ, DIM), BF), shape(SMALL), shape((2, 2, 8, HSEQ))),
        in_specs=vmem(1) + [any_spec()] + vmem(1) + [any_spec()] * 4,
        out_specs=vmem(4),
        scratch_shapes=WBUFS + [pltpu.SemaphoreType.DMA((2, 16)), pltpu.SemaphoreType.DMA((2, 16))],
        compiler_params=comm(1),
        cost_estimate=cost(8 * SEQ * DIM * FFN, 26e6),
        name='bwd')(g, h, small, *weights)


def call_head(n, lab, ids, el, x2, xs, table):
    return pl.pallas_call(
        head_kernel,
        grid=(VSTEPS,),
        out_shape=(shape((SEQ, DIM), BF), shape((2, 8, HSEQ)), shape(PLANE, BF), shape((4, 2, SEQ, DIM), BF)),
        in_specs=[whole((SEQ, DIM)), whole((1, SEQ)), whole((8, SEQ)), whole((SEQ, DIM)), whole((SEQ, DIM)), whole((2, SEQ, DIM)),
                  pl.BlockSpec((VBLK, DIM), lambda i: (i, 0))],
        out_specs=(whole((SEQ, DIM)), whole((2, 8, HSEQ)), any_spec(), any_spec()),
        scratch_shapes=[pltpu.VMEM((DIM, SEQ), F32)] + [pltpu.VMEM((8, SEQ), F32)] * 3 + GSEMS,
        compiler_params=comm(2),
        cost_estimate=cost(4 * SEQ * DIM * VOCAB, VOCAB * DIM * 2, SEQ * VOCAB),
        name='head')(n, lab, ids, el, x2, xs, table)


def call_headgrad(table, n_all, small_all, g0, go):
    toks = 16 * SEQ
    return pl.pallas_call(
        headgrad_kernel,
        grid=(HSTEPS,),
        out_shape=(shape((4, 2, HALF, DIM)), shape(PLANE, BF), shape((4, 2, SEQ, DIM), BF)),
        in_specs=[any_spec(), pl.BlockSpec((HBLK, DIM), lambda i: (i, 0)),
                  pl.BlockSpec((1, 1, 4, 8, HSEQ), lambda i: (i // 4, i % 4, 0, 0, 0)), whole((SEQ, DIM)), whole((2, SEQ, DIM))],
        out_specs=(whole((4, 2, HALF, DIM)), any_spec(), any_spec()),
        scratch_shapes=[pltpu.VMEM((4, WIN, DIM), BF), pltpu.SemaphoreType.DMA((4,))] + GSEMS,
        compiler_params=comm(3),
        cost_estimate=cost(4 * 4 * WIN * DIM * toks, 16e6, 4 * WIN * toks),
        name='headgrad')(table, n_all.reshape(toks, DIM), small_all, g0, go)


def call_wgrad(xg, gg, own_up, own_dn):
    dma = pltpu.SemaphoreType.DMA
    tokens = pltpu.VMEM((4, 2, SEQ, DIM), BF)
    return pl.pallas_call(
        wgrad_kernel,
        out_shape=(shape((4, 4, DRO, DIM)), shape((4, 4, DRO, DIM))),
        in_specs=[any_spec()] * 4,
        out_specs=vmem(2),
        scratch_shapes=[pltpu.VMEM((DIM, CHUNK), BF), pltpu.VMEM((CHUNK, DIM), BF), pltpu.VMEM((DIM, CHUNK), F32),
                        pltpu.VMEM((CHUNK, DIM), F32), tokens, tokens, dma((2,)), dma((4,)), dma((4,))],
        cost_estimate=cost(8 * 2048 * DIM * CHUNK, 16e6),
        name='wgrad')(xg, gg, own_up, own_dn)


def plane_bufs():
    return [pltpu.VMEM((2, 2, DRO, DIM), F32), pltpu.VMEM((2, 4, DRO, DIM), F32), pltpu.VMEM((2, 2, DRO, DIM), F32),
            pltpu.VMEM((4, DRO, DIM), F32), pltpu.VMEM((2, 24, DIM), F32), pltpu.VMEM((2, DRO, DIM), F32), pltpu.VMEM((2, 24, DIM), F32)]


def call_final(part, g_all, small_all, d_up, d_dn):
    dma = pltpu.SemaphoreType.DMA
    return pl.pallas_call(
        final_kernel,
        out_shape=(shape((2, HALF, DIM)), shape((4, URO, DIM)), shape((DRO, DIM))),
        in_specs=[any_spec()] * 2 + vmem(3),
        out_specs=vmem(3),
        scratch_shapes=[pltpu.VMEM((4, 2, HALF, DIM), F32), pltpu.VMEM((16 * SEQ, DIM), BF), dma((6,)), pltpu.VMEM((4, 2, HALF, DIM), F32), pltpu.VMEM((4, HALF, DIM), F32), pltpu.VMEM((SPLIT, DIM), F32),
                        pltpu.VMEM((HALF - SPLIT, DIM), F32), pltpu.VMEM((2, HALF, DIM), F32), pltpu.VMEM((HALF, DIM), F32),
                        pltpu.VMEM((HALF, DIM), F32), pltpu.VMEM((4, URO, DIM), F32), pltpu.VMEM((4, URO, DIM), F32)]
        + plane_bufs() + plane_bufs() + [dma((2, URO)), dma((2, URO)), dma((2, SUBL)), dma((2, SUBL)), dma((2, SUBL)), dma((2,))],
        compiler_params=comm(4),
        cost_estimate=cost(2 * 4 * WIN * DIM * 4096, 20e6),
        name='final')(part, g_all.reshape(16 * SEQ, DIM), small_all, d_up, d_dn)


SWAP = [(0, 1), (1, 0)]


def step_program(token_rows, label_rows, table, up_block, down_block):
    me = lax.axis_index('stage')
    iz, iy, ix = lax.axis_index('z'), lax.axis_index('y'), lax.axis_index('x')
    own_up, own_dn = up_block[0], down_block[0]
    oth_up = lax.ppermute(own_up, 'stage', SWAP)
    oth_dn = lax.ppermute(own_dn, 'stage', SWAP)
    weights = (own_up, own_dn, oth_up, oth_dn)
    tok = lax.dynamic_index_in_dim(token_rows, me, 0, keepdims=False)
    lab = lax.dynamic_index_in_dim(label_rows, me, 0, keepdims=False)
    ids = jnp.concatenate([lab[None], lab[None]] + [tok[None]] * 6, axis=0).astype(F32)
    rows = table[jnp.concatenate([tok, lab])]
    x0, el = rows[:SEQ], rows[SEQ:]
    xs, x2, n, h = call_fwd(x0, *weights)
    gtop, small, n_all, xg = call_head(n, lab[None], ids, el, x2, xs, table)
    go, g0, small_all, pair = call_bwd(gtop, h, small, *weights)
    part, g_all, gg = call_headgrad(table, n_all, small_all, g0, go)
    d_up, d_dn = call_wgrad(xg, gg, own_up, own_dn)
    both, up_parts, grad_down = call_final(part, g_all, small_all, d_up, d_dn)
    grad_up = up_parts.transpose(1, 0, 2).reshape(1, URO, FFN)
    owner = (iz * 4 + iy) * 4 + ix
    begin = jnp.minimum(owner * ROWS // 16 * 16, VOCAB - WIN)
    grad_table = lax.dynamic_slice_in_dim(both.reshape(WIN, DIM), owner * ROWS - begin, ROWS, 0)
    losses = jnp.mean(pair[:, :, 3, :], axis=(1, 2))
    return losses, grad_table, grad_up, grad_down[None]


def solution(mesh):
    fine = jax.sharding.Mesh(mesh.devices.reshape(1, 4, 4, 4, 2), AXES)
    data = ('z', 'y', 'x')
    rows_spec = P(('pod',) + data, None)
    return jax.shard_map(step_program, mesh=fine,
                         in_specs=(rows_spec, rows_spec, P(None, None), P('stage', None, None), P('stage', None, None)),
                         out_specs=(P(('pod',) + data), rows_spec, P(('pod', 'stage'), data, None), P(('pod', 'stage'), data, None)),
                         check_vma=False)
```

```python
import itertools
import math

import jax
import jax.numpy as jnp
from jax import lax
from jax.experimental import pallas as pl
from jax.experimental.pallas import tpu as pltpu
from jax.sharding import PartitionSpec as P

NORM_EPS = 1e-6
BF = jnp.bfloat16
F32 = jnp.float32
VOCAB = 32128
DIM = 768
FFN = 3072
SEQ = 256
CHUNK = 768
NCH = FFN // CHUNK
ROWS = 502
WIN = 528
HALF = WIN // 2
SCALE = DIM ** -0.5
LOG2E = math.log2(math.e)
C2 = SCALE * LOG2E
GC = math.sqrt(2.0 / math.pi)
GA = 0.044715
VBLK = 4096
VSUB = 256
TBLK = 1024
VSTEPS = -(-VOCAB // VBLK)
HBLK = 512
HSTEPS = 16 * SEQ // HBLK
SPLIT = 136
URO = 12
DRO = 48
HSEQ = SEQ // 2
LANES = 128
SUBL = 8
LSE, LAB, TOK, CE = range(4)
ONE, OTHER = range(2)
SIDES = range(4)
AXES = ('pod', 'z', 'y', 'x', 'stage')

AHEAD = 3
NT = (((1,), (1,)), ((), ()))
NN = (((1,), (0,)), ((), ()))
TN = (((0,), (0,)), ((), ()))


def dot(a, b, dims):
    return lax.dot_general(a, b, dims, preferred_element_type=F32)


def rows(fn, v):
    return fn(v, axis=-1, keepdims=True)


def cols(fn, v):
    return fn(v, axis=0, keepdims=True)


def inv_rms(wide):
    return lax.rsqrt(rows(jnp.mean, wide * wide) + NORM_EPS)


def column(row):
    return jnp.transpose(jnp.broadcast_to(row, (LANES, SEQ)))[:, :1]


def across(col):
    return jnp.transpose(jnp.broadcast_to(col, (SEQ, LANES)))[:SUBL]


def pair(sems, k):
    return sems.at[ONE, k], sems.at[OTHER, k]


def whole(dims):
    return pl.BlockSpec(dims, lambda i: (0,) * len(dims))


def gelu(h):
    return 0.5 * h * (1.0 + jnp.tanh(GC * (h + GA * h * h * h)))


def gelu_grad(h):
    t = jnp.tanh(GC * (h + GA * h * h * h))
    return 0.5 * (1.0 + t) + 0.5 * h * (1.0 - t * t) * (GC * (1.0 + 3.0 * GA * h * h))


def any_spec():
    return pl.BlockSpec(memory_space=pl.ANY)


def weight_copies(me, own_up, own_dn, oth_up, oth_dn, up_buf, dn_buf, sems):
    def up(ref, s, j):
        return pltpu.make_async_copy(ref.at[:, pl.ds(j * CHUNK, CHUNK)], up_buf.at[s, j], sems.at[s, j, 0])

    def dn(ref, s, j):
        return pltpu.make_async_copy(ref.at[pl.ds(j * CHUNK, CHUNK), :], dn_buf.at[s, j], sems.at[s, j, 1])

    def start(s, j):
        @pl.when(me == s)
        def _():
            up(own_up, s, j).start()
            dn(own_dn, s, j).start()

        @pl.when(me != s)
        def _():
            up(oth_up, s, j).start()
            if oth_dn is not None:
                dn(oth_dn, s, j).start()

    def wait(s, j):
        up(own_up, s, j).wait()
        if oth_dn is not None:
            dn(own_dn, s, j).wait()
        else:
            @pl.when(me == s)
            def _():
                dn(own_dn, s, j).wait()

    return start, wait


def mod4(i):
    return lax.rem(i + 8, 4)


def ident(**kw):
    base = {name: lax.axis_index(name) for name in AXES}
    base.update(kw)
    return tuple(base[name] for name in AXES)


def remote(src, dst, send, recv, **kw):
    return pltpu.make_async_remote_copy(src_ref=src, dst_ref=dst, send_sem=send, recv_sem=recv, device_id=ident(**kw),
                                        device_id_type=pl.DeviceIdType.MESH)


def greet(targets):
    barrier = pltpu.get_barrier_semaphore()
    for kw in targets:
        pl.semaphore_signal(barrier, inc=1, device_id=ident(**kw), device_id_type=pl.DeviceIdType.MESH)
    pl.semaphore_wait(barrier, len(targets))


def fwd_kernel(x_ref, own_up, own_dn, oth_up, xs_ref, x2_ref, n_ref, h_hbm, oth_dn, up_buf, dn_buf, sems, h_ref, hsems,
               send, recv, saved):
    me = lax.axis_index('stage')
    start, wait = weight_copies(me, own_up, own_dn, oth_up, None, up_buf, dn_buf, sems)
    seq = list(itertools.product(range(2), range(NCH)))
    for item in seq[:AHEAD]:
        start(*item)
    greet([dict(stage=1 - me)])

    def part(ref, j):
        return ref.at[pl.ds(j * CHUNK, CHUNK), :]

    swaps = [remote(part(own_dn, j), dn_buf.at[me, j], send.at[j], recv.at[j], stage=1 - me) for j in range(NCH)]
    saves = [pltpu.make_async_copy(dn_buf.at[1 - me, j], part(oth_dn, j), saved.at[j]) for j in range(NCH)]
    for copy in swaps:
        copy.start()
    x = x_ref[...]
    kept = []
    for s in range(2):
        xs_ref[s] = x
        acc = x.astype(F32)
        for j in range(NCH):
            for item in seq[s * NCH + j + AHEAD:][:1]:
                start(*item)
            wait(s, j)
            h = dot(x, up_buf[s, j], NN)
            h_ref[s, j] = h
            keep = pltpu.make_async_copy(h_ref.at[s, j], h_hbm.at[s, j], hsems.at[s, j])
            keep.start()
            kept.append(keep)
            gated = gelu(h).astype(BF)

            @pl.when(me != s)
            def _(j=j):
                swaps[j].wait_recv()
                saves[j].start()

            acc = acc + dot(gated, dn_buf[s, j], NN)
        x = acc.astype(BF)
    x2_ref[...] = x
    wide = x.astype(F32)
    n_ref[...] = (wide * inv_rms(wide)).astype(BF)
    for keep in kept + saves:
        keep.wait()
    for copy in swaps:
        copy.wait_send()


def bwd_kernel(g_ref, h_hbm, small_ref, own_up, own_dn, oth_up, oth_dn, go_ref, g0_ref, all_ref, pair_ref,
               up_buf, dn_buf, sems, h_ref, hsems, send, recv):
    me = lax.axis_index('stage')
    iy, ix = lax.axis_index('y'), lax.axis_index('x')
    start, wait = weight_copies(me, own_up, own_dn, oth_up, oth_dn, up_buf, dn_buf, sems)
    def take(s, j):
        return pltpu.make_async_copy(h_hbm.at[s, j], h_ref.at[s, j], hsems.at[s, j])

    seq = list(itertools.product((OTHER, ONE), range(NCH)))

    def issue(i):
        for item in seq[i:][:1]:
            start(*item)
            take(*item).start()

    for i in range(AHEAD):
        issue(i)
    peers = [dict(y=mod4(iy + k // 4), x=mod4(ix + k % 4)) for k in range(1, 16)]
    targets = peers + [dict(stage=1 - me)]
    barrier = pltpu.get_barrier_semaphore()
    for kw in targets:
        pl.semaphore_signal(barrier, inc=1, device_id=ident(**kw), device_id_type=pl.DeviceIdType.MESH)
    copies = [remote(small_ref, pair_ref.at[me], send.at[ONE, 15], recv.at[ONE, 15], stage=1 - me)]
    for half, spot in enumerate(((iy, ix), (ix, iy))):
        copies += [remote(small_ref.at[half], all_ref.at[(half,) + spot], send.at[half, k], recv.at[half, k], **kw) for k, kw in enumerate(peers)]
    g = g_ref[...]
    for s in (1, 0):
        go_ref[s] = g
        acc = g.astype(F32)
        for j in range(NCH):
            issue(seq.index((s, j)) + AHEAD)
            wait(s, j)
            gg = dot(g, dn_buf[s, j], NT).astype(BF).astype(F32)
            take(s, j).wait()
            gh = (gg * gelu_grad(h_ref[s, j])).astype(BF)
            acc = acc + dot(gh, up_buf[s, j], NT)
        g = acc.astype(BF)
        if s == 1:
            pl.semaphore_wait(barrier, len(targets))
            for copy in copies:
                copy.start()
    g0_ref[...] = g
    all_ref[ONE, iy, ix] = small_ref[ONE]
    all_ref[OTHER, ix, iy] = small_ref[OTHER]
    pair_ref[me] = small_ref[...]
    for copy in copies:
        copy.wait()


class PlaneGather:
    def __init__(self, src, dst, local, send, recv):
        iy, ix = lax.axis_index('y'), lax.axis_index('x')
        yu, yd, xu, xd = mod4(iy + 1), mod4(iy - 1), mod4(ix + 1), mod4(ix - 1)
        self.targets = [dict(y=yu), dict(y=yd), dict(x=xu), dict(x=xd)]
        self.send, self.recv = send, recv
        self.own, self.phases = [], [[] for _ in range(6)]
        parts = ((iy, ix, 'x', xu, xd, 'y', yu, yd), (ix, iy, 'y', yu, yd, 'x', xu, xd))
        for half, (a, b, near, bu, bd, wide, au, ad) in enumerate(parts):
            self.k = 16 * half
            block = src.at[pl.ds(half * HSEQ, HSEQ), :]
            lo, hi = pl.ds(0, HSEQ // 2), pl.ds(HSEQ // 2, HSEQ // 2)
            out = dst.at[half]
            self.own.append(pltpu.make_async_copy(block, out.at[a, b], local.at[half]))
            left, right = out.at[ad, pl.ds(0, 2)], out.at[au, pl.ds(2, 2)]
            low, high = out.at[a, bd, lo], out.at[a, bu, hi]
            far = mod4(b + 2)
            steps = ((ONE, block, out.at[a, b], block, near, bu, bd), (OTHER, low, low, high, near, bu, bd),
                     (4, block, out.at[a, b], block, wide, au, ad), (5, out.at[a, bd], out.at[a, bd], out.at[a, bd], wide, au, ad),
                     (5, out.at[a, bu], out.at[a, bu], out.at[a, bu], wide, au, ad),
                     (2, out.at[a, far], out.at[a, far], out.at[a, far], wide, au, ad), (3, left, left, right, wide, au, ad))
            for phase, one, dst_one, two, name, upward, downward in steps:
                dst_two = out.at[a, b] if two is block else two
                self.phases[phase] += [self.copy(one, dst_one, name, upward), self.copy(two, dst_two, name, downward)]

    def copy(self, src, dst, name, target):
        self.k += 1
        return remote(src, dst, self.send.at[self.k - 1], self.recv.at[self.k - 1], **{name: target})

    def go(self, phase):
        near, relay, far, last, own, sides = self.phases
        starts = (self.own + near + own, relay + sides, far, last, [])
        waits = ([], near + self.own, relay, own + sides + far, last)
        for copy in waits[phase]:
            copy.wait()
        for copy in starts[phase]:
            copy.start()


class ZGather:
    def __init__(self, src, dst, local, send, recv):
        me, iz = lax.axis_index('stage'), lax.axis_index('z')
        up, down = mod4(iz + 1), mod4(iz - 1)
        self.targets = [dict(stage=1 - me), dict(z=up), dict(z=down)]
        self.own = pltpu.make_async_copy(src.at[me], dst.at[iz, me], local)
        self.swap = remote(src.at[1 - me], dst.at[iz, me], send.at[4], recv.at[4], stage=1 - me)
        moves = ((dst.at[iz], dict(z=up)), (dst.at[iz], dict(z=down)), (dst.at[down, ONE], dict(z=up)), (dst.at[up, OTHER], dict(z=down)))
        moves = [remote(ref, ref, send.at[k], recv.at[k], **kw) for k, (ref, kw) in enumerate(moves)]
        self.first, self.second = moves[:2], moves[2:]

    def begin(self):
        self.swap.start()
        self.own.start()

    def spread(self):
        self.swap.wait()
        self.own.wait()
        for copy in self.first:
            copy.start()

    def forward(self):
        for copy in self.first:
            copy.wait()
        for copy in self.second:
            copy.start()

    def end(self):
        for copy in self.second:
            copy.wait()


def gather_hooks(step, plane, depth):
    @pl.when(step == 0)
    def _():
        greet(plane.targets + depth.targets)
        plane.go(0)
        depth.begin()

    @pl.when(step == 1)
    def _():
        plane.go(1)
        depth.spread()

    @pl.when(step == 3)
    def _():
        plane.go(2)

    @pl.when(step == 6)
    def _():
        plane.go(3)
        depth.forward()


def head_kernel(n_ref, lab_ref, ids_ref, el_ref, x2_ref, xs_ref, e_ref, gtop_ref, small_ref, nall_ref, xg_ref,
                acc_ref, m_ref, s_ref, pk_ref, local, send, recv, zlocal, zsend, zrecv):
    step = pl.program_id(0)
    plane = PlaneGather(n_ref, nall_ref, local, send, recv)
    depth = ZGather(xs_ref, xg_ref, zlocal, zsend, zrecv)
    gather_hooks(step, plane, depth)

    @pl.when(step == 0)
    def _():
        pk = across(rows(jnp.sum, n_ref[...].astype(F32) * el_ref[...].astype(F32)) * C2)
        pk_ref[...] = pk
        m_ref[...] = pk
        s_ref[...] = jnp.zeros_like(s_ref)
        acc_ref[...] = jnp.zeros_like(acc_ref)

    def run(count):
        n = n_ref[...]
        rel = lab_ref[...] - step * VBLK
        m = m_ref[:1, :]
        s = s_ref[:1, :]
        spans = [slice(lo, min(lo + VSUB, count)) for lo in range(0, count, VSUB)]
        ahead = dot(e_ref[spans[ONE], :], n, NT)
        for span, later in zip(spans, spans[1:] + [None]):
            l = ahead
            if later is not None:
                ahead = dot(e_ref[later, :], n, NT)
            new = jnp.maximum(m, cols(jnp.max, l) * C2)
            p = jnp.exp2(l * C2 - new)
            hit = lax.broadcasted_iota(jnp.int32, l.shape, 0) + span.start == rel
            p = jnp.where(hit, 0.0, p)
            alpha = jnp.exp2(m - new)
            s = s * alpha + cols(jnp.sum, p)
            acc_ref[...] = acc_ref[...] * alpha + dot(e_ref[span, :], p.astype(BF), TN)
            m = new
        m_ref[...] = jnp.broadcast_to(m, m_ref.shape)
        s_ref[...] = jnp.broadcast_to(s, s_ref.shape)

    @pl.when(step != VSTEPS - 1)
    def _():
        run(VBLK)

    @pl.when(step == VSTEPS - 1)
    def _():
        run(VOCAB % VBLK)
        m = m_ref[:1, :]
        s = s_ref[:1, :]
        pk = pk_ref[:1, :]
        total = s + jnp.exp2(pk - m)
        lse2 = m + jnp.log2(total)
        ce = (lse2 - pk) * (1.0 / LOG2E)
        row = lax.broadcasted_iota(jnp.int32, ids_ref.shape, 0)
        small = jnp.where(row == LSE, lse2, jnp.where(row == CE, ce, ids_ref[...]))
        small_ref[ONE] = small[:, :HSEQ]
        small_ref[OTHER] = small[:, HSEQ:]
        inv_total = 1.0 / total
        gn = jnp.transpose(acc_ref[...] * inv_total) - column(s * inv_total) * el_ref[...].astype(F32)
        gn = (gn * SCALE).astype(BF).astype(F32)
        wide = x2_ref[...].astype(F32)
        inv = inv_rms(wide)
        nw = wide * inv
        inner = rows(jnp.mean, gn * nw)
        gtop_ref[...] = (inv * (gn - nw * inner)).astype(BF)
        plane.go(4)
        depth.end()


def window_start(seg):
    owner = (seg * 4 + lax.axis_index('y')) * 4 + lax.axis_index('x')
    return jnp.minimum(owner * ROWS // 16 * 16, VOCAB - WIN)


def headgrad_kernel(table_ref, n_ref, all_ref, g0_ref, go_ref, out_ref, gall_ref, gg_ref, e_buf, sems,
                    local, send, recv, zlocal, zsend, zrecv):
    step = pl.program_id(0)
    plane = PlaneGather(g0_ref, gall_ref, local, send, recv)
    depth = ZGather(go_ref, gg_ref, zlocal, zsend, zrecv)

    def copy(seg):
        src = table_ref.at[pl.ds(pl.multiple_of(window_start(seg), 16), WIN), :]
        return pltpu.make_async_copy(src, e_buf.at[seg], sems.at[seg])

    @pl.when(step == 0)
    def _():
        for seg in SIDES:
            copy(seg).start()

    gather_hooks(step, plane, depth)

    @pl.when(step == 0)
    def _():
        out_ref[...] = jnp.zeros_like(out_ref)
        for seg in SIDES:
            copy(seg).wait()

    n = n_ref[...]
    def line(which):
        return jnp.concatenate([all_ref[ONE, ONE, q, pl.ds(which, 1), :] for q in SIDES], axis=1)

    lse = line(LSE) - math.log2(SCALE)
    lab = line(LAB).astype(jnp.int32)
    row = lax.broadcasted_iota(jnp.int32, (WIN, HBLK), 0)
    ahead = dot(e_buf[ONE], n, NT)
    for seg in SIDES:
        l = ahead
        if seg + 1 < len(SIDES):
            ahead = dot(e_buf[seg + 1], n, NT)
        p = jnp.exp2(l * C2 - lse)
        g = (p - jnp.where(row == lab - window_start(seg), SCALE, 0.0)).astype(BF)
        d = dot(g, n, NN)
        out_ref[seg, ONE] += d[:HALF]
        out_ref[seg, OTHER] += d[HALF:]

    @pl.when(step == HSTEPS - 1)
    def _():
        plane.go(4)
        depth.end()


def wgrad_kernel(xg_ref, gg_ref, up_ref, dn_ref, out_up, out_dn, wu, wd, acc_up, acc_dn, xbuf, gbuf, sems, xsems, gsems):
    iz = lax.axis_index('z')
    first = pl.multiple_of(iz * CHUNK, CHUNK)
    cu = pltpu.make_async_copy(up_ref.at[:, pl.ds(first, CHUNK)], wu, sems.at[ONE])
    cd = pltpu.make_async_copy(dn_ref.at[pl.ds(first, CHUNK), :], wd, sems.at[OTHER])
    loads = [(pltpu.make_async_copy(xg_ref.at[q], xbuf.at[q], xsems.at[q]), pltpu.make_async_copy(gg_ref.at[q], gbuf.at[q], gsems.at[q])) for q in SIDES]
    cu.start()
    cd.start()
    for copy in loads[ONE]:
        copy.start()
    cu.wait()
    for q in SIDES:
        for some in loads[q + 1:][:1]:
            for copy in some:
                copy.start()
        for copy in loads[q]:
            copy.wait()
        if q == ONE:
            cd.wait()
        x = xbuf[q].reshape(2 * SEQ, DIM)
        g = gbuf[q].reshape(2 * SEQ, DIM)
        hid = dot(x, wu[...], NN)
        gg = dot(g, wd[...], NT).astype(BF).astype(F32)
        gated = gelu(hid).astype(BF)
        gh = (gg * gelu_grad(hid)).astype(BF)
        du = dot(x, gh, TN)
        dd = dot(gated, g, TN)
        acc_up[...] = acc_up[...] + du if q else du
        acc_dn[...] = acc_dn[...] + dd if q else dd
    for kz, ky, kx in itertools.product(SIDES, SIDES, SIDES):
        out_up[kx, ky, pl.ds(URO * kz, URO), :] = acc_up[pl.ds(URO * ((kz * 4 + ky) * 4 + kx), URO), :]
    for ky, kx in itertools.product(SIDES, SIDES):
        out_dn[ky, kx] = acc_dn[pl.ds(DRO * (ky * 4 + kx), DRO), :]


class PlaneReduce:
    def __init__(self, src, first, second, bufs, sems):
        self.src, self.bufs, self.sems = src, bufs, sems
        self.first, self.second = first, second

    def axis(self, name):
        i = lax.axis_index(name)
        return i, mod4(i + 1), mod4(i - 1), mod4(i + 2)

    def sem(self, k):
        return pair(self.sems, k)

    def pieces(self, phase):
        rel1, fin1, snd1, total, rel2, fin2, snd2 = self.bufs
        if phase == 0:
            name, src, rel, fin, snd, half, base = self.first, self.src, rel1, fin1, snd1, 2, 0
        else:
            name, src, rel, fin, snd, half, base = self.second, total, rel2, fin2, snd2, 24, 6
        i, up, down, far = self.axis(name)
        lo, hi = pl.ds(0, half), pl.ds(half, half)
        to_up, to_down = {name: up}, {name: down}
        moves = ((src.at[far, lo], rel.at[ONE], to_up), (src.at[far, hi], rel.at[OTHER], to_down),
                 (src.at[up, hi], fin.at[ONE, hi], to_up), (src.at[down, lo], fin.at[OTHER, lo], to_down),
                 (snd.at[ONE], fin.at[ONE, lo], to_up), (snd.at[OTHER], fin.at[OTHER, hi], to_down))
        moves = [remote(a, b, *self.sem(base + k), **kw) for k, (a, b, kw) in enumerate(moves)]
        early, late = moves[:4], moves[4:]
        return i, up, down, lo, hi, src, rel, fin, snd, early, late

    def start(self, phase):
        for copy in self.pieces(phase)[-2]:
            copy.start()

    def relay(self, phase):
        i, up, down, lo, hi, src, rel, fin, snd, early, late = self.pieces(phase)
        for side, part in enumerate((src.at[up, lo], src.at[down, hi])):
            early[side].wait_recv()
            snd[side] = part[...] + rel[side]
            late[side].start()

    def finish(self, phase):
        i, up, down, lo, hi, src, rel, fin, snd, early, late = self.pieces(phase)
        for copy in early[2:] + late:
            copy.wait_recv()
        return src[i] + fin[ONE] + fin[OTHER]

    def drain(self, phase):
        early, late = self.pieces(phase)[-2:]
        for copy in early + late:
            copy.wait_send()


def final_kernel(part_hbm, g_hbm, all_ref, up_ref, dn_ref, tab_ref, upo_ref, dno_ref,
                 part_ref, g_ref, lsems, t_ref, swap_ref, zrel0, zrel1, zfin, mine, theirs, u4, ugot, *rest):
    bufs_a, bufs_b, (sems_a, sems_b, sems_c, sems_z, sems_u, sems_f) = rest[:7], rest[7:14], rest[14:]
    me, iz, iy, ix = (lax.axis_index(name) for name in ('stage', 'z', 'y', 'x'))
    up, down, far = mod4(iz + 1), mod4(iz - 1), mod4(iz + 2)
    order = (far, up, down, iz)
    load = pltpu.make_async_copy(g_hbm, g_ref, lsems.at[4])
    pieces = [pltpu.make_async_copy(part_hbm.at[seg], part_ref.at[k], lsems.at[k]) for k, seg in enumerate(order)]
    load.start()
    pieces[ONE].start()
    greet([dict(stage=1 - me), dict(z=up), dict(z=down), dict(z=far), dict(y=mod4(iy + 1)), dict(y=mod4(iy - 1)),
           dict(x=mod4(ix + 1)), dict(x=mod4(ix - 1))])
    red_a = PlaneReduce(up_ref, 'x', 'y', bufs_a, sems_a)
    red_b = PlaneReduce(dn_ref, 'y', 'x', bufs_b, sems_b)
    red_a.start(ONE)
    red_b.start(ONE)
    total_a, total_b = bufs_a[3], bufs_b[3]
    swaps = [remote(t_ref.at[seg, 1 - me], swap_ref.at[k], *pair(sems_c, k), stage=1 - me) for k, seg in enumerate(order)]
    lo, hi = pl.ds(0, SPLIT), pl.ds(SPLIT, HALF - SPLIT)

    to_up, to_down = dict(z=up), dict(z=down)
    moves = ((t_ref.at[far, me, lo], zrel0, to_up), (t_ref.at[far, me, hi], zrel1, to_down),
             (t_ref.at[up, me, hi], zfin.at[ONE, hi], to_up), (t_ref.at[up, me, lo], zfin.at[ONE, lo], to_up),
             (t_ref.at[down, me, lo], zfin.at[OTHER, lo], to_down), (t_ref.at[down, me, hi], zfin.at[OTHER, hi], to_down))
    moves = [remote(a, b, *pair(sems_z, k), **kw) for k, (a, b, kw) in enumerate(moves)]
    rel_up, rel_down, up_hi, up_lo, down_lo, down_hi = moves

    def embed(k, half):
        seg = order[k]
        row = lax.broadcasted_iota(jnp.int32, (HALF, TBLK), 0) + (window_start(seg) + half * HALF)
        for b in SIDES:
            blocks = [divmod(SUBL * b + q, 4) for q in range(SUBL)]
            tok = jnp.concatenate([all_ref[i // 4, i % 4, q, pl.ds(TOK, 1), :] for i, q in blocks], axis=1).astype(jnp.int32)
            hot = jnp.where(row == tok, 1.0, 0.0).astype(BF)
            d = dot(hot, g_ref[b * TBLK:(b + 1) * TBLK, :], NN)
            base = t_ref.at[seg] if b else part_ref.at[k]
            t_ref[seg, half] = base[half] + d

    def settle(k):
        pieces[k].wait()
        embed(k, 1 - me)
        swaps[k].start()
        embed(k, me)
        swaps[k].wait_recv()
        t_ref[order[k], me] += swap_ref[k]

    ifar, iup, idown, iown = SIDES
    load.wait()
    for copy in pieces[1:]:
        copy.start()
    settle(ifar)
    rel_up.start()
    rel_down.start()
    settle(iup)
    up_hi.start()
    red_a.relay(ONE)
    red_b.relay(ONE)
    settle(idown)
    down_lo.start()
    rel_up.wait_recv()
    t_ref[up, me, lo] += zrel0[...]
    up_lo.start()
    rel_down.wait_recv()
    t_ref[down, me, hi] += zrel1[...]
    down_hi.start()
    settle(iown)
    total_a[...] = red_a.finish(ONE)
    red_a.start(OTHER)
    total_b[...] = red_b.finish(ONE)
    red_b.start(OTHER)
    red_a.relay(OTHER)
    red_b.relay(OTHER)
    total = red_a.finish(OTHER)
    for k in SIDES:
        u4[k] = total[URO * k:URO * (k + 1), :]
    turns = [remote(u4.at[mod4(iz + k)], ugot.at[iz], *pair(sems_u, k), z=mod4(iz + k)) for k in SIDES[1:]]
    for copy in turns:
        copy.start()
    dno_ref[...] = red_b.finish(OTHER)
    for copy in (up_hi, up_lo, down_lo, down_hi):
        copy.wait_recv()
    mine[...] = t_ref[iz, me] + zfin[ONE] + zfin[OTHER]
    back = remote(mine, theirs, sems_f.at[ONE], sems_f.at[OTHER], stage=1 - me)
    back.start()
    tab_ref[me] = mine[...]
    for copy in turns:
        copy.wait_recv()
    upo_ref[...] = ugot[...]
    upo_ref[iz] = u4[iz]
    back.wait_recv()
    tab_ref[1 - me] = theirs[...]
    for copy in swaps + moves + [back] + turns:
        copy.wait_send()
    for phase in (ONE, OTHER):
        red_a.drain(phase)
        red_b.drain(phase)


def cost(flops, nbytes, trans=0):
    return pl.CostEstimate(flops=int(flops), bytes_accessed=int(nbytes), transcendentals=int(trans))


def vmem(n):
    return [pl.BlockSpec(memory_space=pltpu.VMEM)] * n


def shape(dims, dtype=F32):
    return jax.ShapeDtypeStruct(dims, dtype)


def comm(cid):
    return pltpu.CompilerParams(collective_id=cid, has_side_effects=True)


WBUFS = [pltpu.VMEM((2, NCH, DIM, CHUNK), BF), pltpu.VMEM((2, NCH, CHUNK, DIM), BF), pltpu.SemaphoreType.DMA((2, NCH, 2)),
         pltpu.VMEM((2, NCH, SEQ, CHUNK), F32), pltpu.SemaphoreType.DMA((2, NCH))]
HID = (2, NCH, SEQ, CHUNK)
GSEMS = [pltpu.SemaphoreType.DMA((2,)), pltpu.SemaphoreType.DMA((32,)), pltpu.SemaphoreType.DMA((32,)),
         pltpu.SemaphoreType.DMA, pltpu.SemaphoreType.DMA((5,)), pltpu.SemaphoreType.DMA((5,))]
PLANE = (2, 4, 4, SEQ // 2, DIM)
SMALL = (2, 4, 4, 8, SEQ // 2)


def call_fwd(x, *weights):
    tok = shape((SEQ, DIM), BF)
    dma = pltpu.SemaphoreType.DMA
    return pl.pallas_call(
        fwd_kernel,
        out_shape=(shape((2, SEQ, DIM), BF), tok, tok, shape(HID), shape((FFN, DIM), BF)),
        in_specs=vmem(1) + [any_spec()] * 3,
        out_specs=vmem(3) + [any_spec()] * 2,
        scratch_shapes=WBUFS + [dma((NCH,))] * 3,
        compiler_params=comm(5),
        cost_estimate=cost(8 * SEQ * DIM * FFN, 26e6),
        name='fwd')(x, *weights)


def call_bwd(g, h, small, *weights):
    return pl.pallas_call(
        bwd_kernel,
        out_shape=(shape((2, SEQ, DIM), BF), shape((SEQ, DIM), BF), shape(SMALL), shape((2, 2, 8, HSEQ))),
        in_specs=vmem(1) + [any_spec()] + vmem(1) + [any_spec()] * 4,
        out_specs=vmem(4),
        scratch_shapes=WBUFS + [pltpu.SemaphoreType.DMA((2, 16)), pltpu.SemaphoreType.DMA((2, 16))],
        compiler_params=comm(1),
        cost_estimate=cost(8 * SEQ * DIM * FFN, 26e6),
        name='bwd')(g, h, small, *weights)


def call_head(n, lab, ids, el, x2, xs, table):
    return pl.pallas_call(
        head_kernel,
        grid=(VSTEPS,),
        out_shape=(shape((SEQ, DIM), BF), shape((2, 8, HSEQ)), shape(PLANE, BF), shape((4, 2, SEQ, DIM), BF)),
        in_specs=[whole((SEQ, DIM)), whole((1, SEQ)), whole((8, SEQ)), whole((SEQ, DIM)), whole((SEQ, DIM)), whole((2, SEQ, DIM)),
                  pl.BlockSpec((VBLK, DIM), lambda i: (i, 0))],
        out_specs=(whole((SEQ, DIM)), whole((2, 8, HSEQ)), any_spec(), any_spec()),
        scratch_shapes=[pltpu.VMEM((DIM, SEQ), F32)] + [pltpu.VMEM((8, SEQ), F32)] * 3 + GSEMS,
        compiler_params=comm(2),
        cost_estimate=cost(4 * SEQ * DIM * VOCAB, VOCAB * DIM * 2, SEQ * VOCAB),
        name='head')(n, lab, ids, el, x2, xs, table)


def call_headgrad(table, n_all, small_all, g0, go):
    toks = 16 * SEQ
    return pl.pallas_call(
        headgrad_kernel,
        grid=(HSTEPS,),
        out_shape=(shape((4, 2, HALF, DIM)), shape(PLANE, BF), shape((4, 2, SEQ, DIM), BF)),
        in_specs=[any_spec(), pl.BlockSpec((HBLK, DIM), lambda i: (i, 0)),
                  pl.BlockSpec((1, 1, 4, 8, HSEQ), lambda i: (i // 4, i % 4, 0, 0, 0)), whole((SEQ, DIM)), whole((2, SEQ, DIM))],
        out_specs=(whole((4, 2, HALF, DIM)), any_spec(), any_spec()),
        scratch_shapes=[pltpu.VMEM((4, WIN, DIM), BF), pltpu.SemaphoreType.DMA((4,))] + GSEMS,
        compiler_params=comm(3),
        cost_estimate=cost(4 * 4 * WIN * DIM * toks, 16e6, 4 * WIN * toks),
        name='headgrad')(table, n_all.reshape(toks, DIM), small_all, g0, go)


def call_wgrad(xg, gg, own_up, own_dn):
    dma = pltpu.SemaphoreType.DMA
    tokens = pltpu.VMEM((4, 2, SEQ, DIM), BF)
    return pl.pallas_call(
        wgrad_kernel,
        out_shape=(shape((4, 4, DRO, DIM)), shape((4, 4, DRO, DIM))),
        in_specs=[any_spec()] * 4,
        out_specs=vmem(2),
        scratch_shapes=[pltpu.VMEM((DIM, CHUNK), BF), pltpu.VMEM((CHUNK, DIM), BF), pltpu.VMEM((DIM, CHUNK), F32),
                        pltpu.VMEM((CHUNK, DIM), F32), tokens, tokens, dma((2,)), dma((4,)), dma((4,))],
        cost_estimate=cost(8 * 2048 * DIM * CHUNK, 16e6),
        name='wgrad')(xg, gg, own_up, own_dn)


def plane_bufs():
    return [pltpu.VMEM((2, 2, DRO, DIM), F32), pltpu.VMEM((2, 4, DRO, DIM), F32), pltpu.VMEM((2, 2, DRO, DIM), F32),
            pltpu.VMEM((4, DRO, DIM), F32), pltpu.VMEM((2, 24, DIM), F32), pltpu.VMEM((2, DRO, DIM), F32), pltpu.VMEM((2, 24, DIM), F32)]


def call_final(part, g_all, small_all, d_up, d_dn):
    dma = pltpu.SemaphoreType.DMA
    return pl.pallas_call(
        final_kernel,
        out_shape=(shape((2, HALF, DIM)), shape((4, URO, DIM)), shape((DRO, DIM))),
        in_specs=[any_spec()] * 2 + vmem(3),
        out_specs=vmem(3),
        scratch_shapes=[pltpu.VMEM((4, 2, HALF, DIM), F32), pltpu.VMEM((16 * SEQ, DIM), BF), dma((6,)), pltpu.VMEM((4, 2, HALF, DIM), F32), pltpu.VMEM((4, HALF, DIM), F32), pltpu.VMEM((SPLIT, DIM), F32),
                        pltpu.VMEM((HALF - SPLIT, DIM), F32), pltpu.VMEM((2, HALF, DIM), F32), pltpu.VMEM((HALF, DIM), F32),
                        pltpu.VMEM((HALF, DIM), F32), pltpu.VMEM((4, URO, DIM), F32), pltpu.VMEM((4, URO, DIM), F32)]
        + plane_bufs() + plane_bufs() + [dma((2, URO)), dma((2, URO)), dma((2, SUBL)), dma((2, SUBL)), dma((2, SUBL)), dma((2,))],
        compiler_params=comm(4),
        cost_estimate=cost(2 * 4 * WIN * DIM * 4096, 20e6),
        name='final')(part, g_all.reshape(16 * SEQ, DIM), small_all, d_up, d_dn)


SWAP = [(0, 1), (1, 0)]


def step_program(token_rows, label_rows, table, up_block, down_block):
    me = lax.axis_index('stage')
    iz, iy, ix = lax.axis_index('z'), lax.axis_index('y'), lax.axis_index('x')
    own_up, own_dn = up_block[0], down_block[0]
    oth_up = lax.ppermute(own_up, 'stage', SWAP)
    tok = lax.dynamic_index_in_dim(token_rows, me, 0, keepdims=False)
    lab = lax.dynamic_index_in_dim(label_rows, me, 0, keepdims=False)
    ids = jnp.concatenate([lab[None], lab[None]] + [tok[None]] * 6, axis=0).astype(F32)
    rows = table[jnp.concatenate([tok, lab])]
    x0, el = rows[:SEQ], rows[SEQ:]
    xs, x2, n, h, oth_dn = call_fwd(x0, own_up, own_dn, oth_up)
    weights = (own_up, own_dn, oth_up, oth_dn)
    gtop, small, n_all, xg = call_head(n, lab[None], ids, el, x2, xs, table)
    go, g0, small_all, pair = call_bwd(gtop, h, small, *weights)
    part, g_all, gg = call_headgrad(table, n_all, small_all, g0, go)
    d_up, d_dn = call_wgrad(xg, gg, own_up, own_dn)
    both, up_parts, grad_down = call_final(part, g_all, small_all, d_up, d_dn)
    grad_up = up_parts.transpose(1, 0, 2).reshape(1, URO, FFN)
    owner = (iz * 4 + iy) * 4 + ix
    begin = jnp.minimum(owner * ROWS // 16 * 16, VOCAB - WIN)
    grad_table = lax.dynamic_slice_in_dim(both.reshape(WIN, DIM), owner * ROWS - begin, ROWS, 0)
    losses = jnp.mean(pair[:, :, 3, :], axis=(1, 2))
    return losses, grad_table, grad_up, grad_down[None]


def solution(mesh):
    fine = jax.sharding.Mesh(mesh.devices.reshape(1, 4, 4, 4, 2), AXES)
    data = ('z', 'y', 'x')
    rows_spec = P(('pod',) + data, None)
    return jax.shard_map(step_program, mesh=fine,
                         in_specs=(rows_spec, rows_spec, P(None, None), P('stage', None, None), P('stage', None, None)),
                         out_specs=(P(('pod',) + data), rows_spec, P(('pod', 'stage'), data, None), P(('pod', 'stage'), data, None)),
                         check_vma=False)
```

```python
import itertools
import math

import jax
import jax.numpy as jnp
from jax import lax
from jax.experimental import pallas as pl
from jax.experimental.pallas import tpu as pltpu
from jax.sharding import PartitionSpec as P

NORM_EPS = 1e-6
BF = jnp.bfloat16
F32 = jnp.float32
VOCAB = 32128
DIM = 768
FFN = 3072
SEQ = 256
CHUNK = 768
NCH = FFN // CHUNK
ROWS = 502
WIN = 528
HALF = WIN // 2
SCALE = DIM ** -0.5
LOG2E = math.log2(math.e)
C2 = SCALE * LOG2E
GC = math.sqrt(2.0 / math.pi)
GA = 0.044715
VBLK = 4096
VSUB = 256
TBLK = 1024
VSTEPS = -(-VOCAB // VBLK)
HBLK = 512
HSTEPS = 16 * SEQ // HBLK
SPLIT = 136
URO = 12
DRO = 48
HSEQ = SEQ // 2
LANES = 128
SUBL = 8
LSE, LAB, TOK, CE = range(4)
ONE, OTHER = range(2)
SIDES = range(4)
AXES = ('pod', 'z', 'y', 'x', 'stage')

AHEAD = 3
NT = (((1,), (1,)), ((), ()))
NN = (((1,), (0,)), ((), ()))
TN = (((0,), (0,)), ((), ()))


def dot(a, b, dims):
    return lax.dot_general(a, b, dims, preferred_element_type=F32)


def rows(fn, v):
    return fn(v, axis=-1, keepdims=True)


def cols(fn, v):
    return fn(v, axis=0, keepdims=True)


def inv_rms(wide):
    return lax.rsqrt(rows(jnp.mean, wide * wide) + NORM_EPS)


def column(row):
    return jnp.transpose(jnp.broadcast_to(row, (LANES, SEQ)))[:, :1]


def across(col):
    return jnp.transpose(jnp.broadcast_to(col, (SEQ, LANES)))[:SUBL]


def pair(sems, k):
    return sems.at[ONE, k], sems.at[OTHER, k]


def whole(dims):
    return pl.BlockSpec(dims, lambda i: (0,) * len(dims))


def gelu(h):
    return 0.5 * h * (1.0 + jnp.tanh(GC * (h + GA * h * h * h)))


def gelu_grad(h):
    t = jnp.tanh(GC * (h + GA * h * h * h))
    return 0.5 * (1.0 + t) + 0.5 * h * (1.0 - t * t) * (GC * (1.0 + 3.0 * GA * h * h))


def any_spec():
    return pl.BlockSpec(memory_space=pl.ANY)


def weight_copies(me, own_up, own_dn, oth_up, oth_dn, up_buf, dn_buf, sems):
    def up(ref, s, j):
        return pltpu.make_async_copy(ref.at[:, pl.ds(j * CHUNK, CHUNK)], up_buf.at[s, j], sems.at[s, j, 0])

    def dn(ref, s, j):
        return pltpu.make_async_copy(ref.at[pl.ds(j * CHUNK, CHUNK), :], dn_buf.at[s, j], sems.at[s, j, 1])

    def start(s, j):
        @pl.when(me == s)
        def _():
            up(own_up, s, j).start()
            dn(own_dn, s, j).start()

        @pl.when(me != s)
        def _():
            up(oth_up, s, j).start()
            if oth_dn is not None:
                dn(oth_dn, s, j).start()

    def wait(s, j):
        up(own_up, s, j).wait()
        if oth_dn is not None:
            dn(own_dn, s, j).wait()
        else:
            @pl.when(me == s)
            def _():
                dn(own_dn, s, j).wait()

    return start, wait


def mod4(i):
    return lax.rem(i + 8, 4)


def ident(**kw):
    base = {name: lax.axis_index(name) for name in AXES}
    base.update(kw)
    return tuple(base[name] for name in AXES)


def remote(src, dst, send, recv, **kw):
    return pltpu.make_async_remote_copy(src_ref=src, dst_ref=dst, send_sem=send, recv_sem=recv, device_id=ident(**kw),
                                        device_id_type=pl.DeviceIdType.MESH)


def announce(targets):
    barrier = pltpu.get_barrier_semaphore()
    for kw in targets:
        pl.semaphore_signal(barrier, inc=1, device_id=ident(**kw), device_id_type=pl.DeviceIdType.MESH)


def await_all(targets):
    pl.semaphore_wait(pltpu.get_barrier_semaphore(), len(targets))


def greet(targets):
    announce(targets)
    await_all(targets)


def fwd_kernel(x_ref, own_up, own_dn, oth_up, xs_ref, x2_ref, n_ref, h_hbm, oth_dn, up_buf, dn_buf, sems, h_ref, hsems,
               send, recv, saved):
    me = lax.axis_index('stage')
    start, wait = weight_copies(me, own_up, own_dn, oth_up, None, up_buf, dn_buf, sems)
    seq = list(itertools.product(range(2), range(NCH)))
    for item in seq[:AHEAD]:
        start(*item)
    greet([dict(stage=1 - me)])

    def part(ref, j):
        return ref.at[pl.ds(j * CHUNK, CHUNK), :]

    swaps = [remote(part(own_dn, j), dn_buf.at[me, j], send.at[j], recv.at[j], stage=1 - me) for j in range(NCH)]
    saves = [pltpu.make_async_copy(dn_buf.at[1 - me, j], part(oth_dn, j), saved.at[j]) for j in range(NCH)]
    for copy in swaps:
        copy.start()
    x = x_ref[...]
    kept = []
    for s in range(2):
        xs_ref[s] = x
        acc = x.astype(F32)
        ready = None
        for j in range(NCH + 1):
            if j < NCH:
                for item in seq[s * NCH + j + AHEAD:][:1]:
                    start(*item)
                wait(s, j)
            if j:
                @pl.when(me != s)
                def _(j=j - 1):
                    swaps[j].wait_recv()
                    saves[j].start()

            h, ready = ready, dot(x, up_buf[s, j], NN) if j < NCH else None
            if j:
                acc = acc + dot(gelu(h).astype(BF), dn_buf[s, j - 1], NN)
            if j < NCH:
                h_ref[s, j] = ready
                keep = pltpu.make_async_copy(h_ref.at[s, j], h_hbm.at[s, j], hsems.at[s, j])
                keep.start()
                kept.append(keep)
        x = acc.astype(BF)
    x2_ref[...] = x
    wide = x.astype(F32)
    n_ref[...] = (wide * inv_rms(wide)).astype(BF)
    for keep in kept + saves:
        keep.wait()
    for copy in swaps:
        copy.wait_send()


def bwd_kernel(g_ref, h_hbm, small_ref, own_up, own_dn, oth_up, oth_dn, go_ref, g0_ref, all_ref, pair_ref,
               up_buf, dn_buf, sems, h_ref, hsems, send, recv):
    me = lax.axis_index('stage')
    iy, ix = lax.axis_index('y'), lax.axis_index('x')
    start, wait = weight_copies(me, own_up, own_dn, oth_up, oth_dn, up_buf, dn_buf, sems)
    def take(s, j):
        return pltpu.make_async_copy(h_hbm.at[s, j], h_ref.at[s, j], hsems.at[s, j])

    seq = list(itertools.product((OTHER, ONE), range(NCH)))

    def issue(i):
        for item in seq[i:][:1]:
            start(*item)
            take(*item).start()

    for i in range(AHEAD):
        issue(i)
    peers = [dict(y=mod4(iy + k // 4), x=mod4(ix + k % 4)) for k in range(1, 16)]
    targets = peers + [dict(stage=1 - me)]
    barrier = pltpu.get_barrier_semaphore()
    for kw in targets:
        pl.semaphore_signal(barrier, inc=1, device_id=ident(**kw), device_id_type=pl.DeviceIdType.MESH)
    copies = [remote(small_ref, pair_ref.at[me], send.at[ONE, 15], recv.at[ONE, 15], stage=1 - me)]
    for half, spot in enumerate(((iy, ix), (ix, iy))):
        copies += [remote(small_ref.at[half], all_ref.at[(half,) + spot], send.at[half, k], recv.at[half, k], **kw) for k, kw in enumerate(peers)]
    g = g_ref[...]
    for s in (1, 0):
        go_ref[s] = g
        acc = g.astype(F32)
        ready = None
        for j in range(NCH + 1):
            if j < NCH:
                issue(seq.index((s, j)) + AHEAD)
                wait(s, j)
                take(s, j).wait()
            raw, ready = ready, dot(g, dn_buf[s, j], NT) if j < NCH else None
            if j:
                gh = (raw.astype(BF).astype(F32) * gelu_grad(h_ref[s, j - 1])).astype(BF)
                acc = acc + dot(gh, up_buf[s, j - 1], NT)
        g = acc.astype(BF)
        if s == 1:
            pl.semaphore_wait(barrier, len(targets))
            for copy in copies:
                copy.start()
    g0_ref[...] = g
    all_ref[ONE, iy, ix] = small_ref[ONE]
    all_ref[OTHER, ix, iy] = small_ref[OTHER]
    pair_ref[me] = small_ref[...]
    for copy in copies:
        copy.wait()


class PlaneGather:
    def __init__(self, src, dst, local, send, recv):
        iy, ix = lax.axis_index('y'), lax.axis_index('x')
        yu, yd, xu, xd = mod4(iy + 1), mod4(iy - 1), mod4(ix + 1), mod4(ix - 1)
        self.targets = [dict(y=yu), dict(y=yd), dict(x=xu), dict(x=xd)]
        self.send, self.recv = send, recv
        self.own, self.phases = [], [[] for _ in range(6)]
        parts = ((iy, ix, 'x', xu, xd, 'y', yu, yd), (ix, iy, 'y', yu, yd, 'x', xu, xd))
        for half, (a, b, near, bu, bd, wide, au, ad) in enumerate(parts):
            self.k = 16 * half
            block = src.at[pl.ds(half * HSEQ, HSEQ), :]
            lo, hi = pl.ds(0, HSEQ // 2), pl.ds(HSEQ // 2, HSEQ // 2)
            out = dst.at[half]
            self.own.append(pltpu.make_async_copy(block, out.at[a, b], local.at[half]))
            left, right = out.at[ad, pl.ds(0, 2)], out.at[au, pl.ds(2, 2)]
            low, high = out.at[a, bd, lo], out.at[a, bu, hi]
            far = mod4(b + 2)
            steps = ((ONE, block, out.at[a, b], block, near, bu, bd), (OTHER, low, low, high, near, bu, bd),
                     (4, block, out.at[a, b], block, wide, au, ad), (5, out.at[a, bd], out.at[a, bd], out.at[a, bd], wide, au, ad),
                     (5, out.at[a, bu], out.at[a, bu], out.at[a, bu], wide, au, ad),
                     (2, out.at[a, far], out.at[a, far], out.at[a, far], wide, au, ad), (3, left, left, right, wide, au, ad))
            for phase, one, dst_one, two, name, upward, downward in steps:
                dst_two = out.at[a, b] if two is block else two
                self.phases[phase] += [self.copy(one, dst_one, name, upward), self.copy(two, dst_two, name, downward)]

    def copy(self, src, dst, name, target):
        self.k += 1
        return remote(src, dst, self.send.at[self.k - 1], self.recv.at[self.k - 1], **{name: target})

    def go(self, phase):
        near, relay, far, last, own, sides = self.phases
        starts = (self.own + near + own, relay + sides, far, last, [])
        waits = ([], near + self.own, relay, own + sides + far, last)
        for copy in waits[phase]:
            copy.wait()
        for copy in starts[phase]:
            copy.start()


class ZGather:
    def __init__(self, src, dst, local, send, recv):
        me, iz = lax.axis_index('stage'), lax.axis_index('z')
        up, down = mod4(iz + 1), mod4(iz - 1)
        self.targets = [dict(stage=1 - me), dict(z=up), dict(z=down)]
        self.own = pltpu.make_async_copy(src.at[me], dst.at[iz, me], local)
        self.swap = remote(src.at[1 - me], dst.at[iz, me], send.at[4], recv.at[4], stage=1 - me)
        moves = ((dst.at[iz], dict(z=up)), (dst.at[iz], dict(z=down)), (dst.at[down, ONE], dict(z=up)), (dst.at[up, OTHER], dict(z=down)))
        moves = [remote(ref, ref, send.at[k], recv.at[k], **kw) for k, (ref, kw) in enumerate(moves)]
        self.first, self.second = moves[:2], moves[2:]

    def begin(self):
        self.swap.start()
        self.own.start()

    def spread(self):
        self.swap.wait()
        self.own.wait()
        for copy in self.first:
            copy.start()

    def forward(self):
        for copy in self.first:
            copy.wait()
        for copy in self.second:
            copy.start()

    def end(self):
        for copy in self.second:
            copy.wait()


def gather_hooks(step, plane, depth):
    targets = plane.targets + depth.targets

    @pl.when(step == 0)
    def _():
        announce(targets)

    @pl.when(step == 1)
    def _():
        await_all(targets)
        plane.go(0)
        depth.begin()

    @pl.when(step == 2)
    def _():
        plane.go(1)
        depth.spread()

    @pl.when(step == 4)
    def _():
        plane.go(2)

    @pl.when(step == 6)
    def _():
        plane.go(3)
        depth.forward()


def head_kernel(n_ref, lab_ref, ids_ref, el_ref, x2_ref, xs_ref, e_ref, gtop_ref, small_ref, nall_ref, xg_ref,
                acc_ref, m_ref, s_ref, pk_ref, local, send, recv, zlocal, zsend, zrecv):
    step = pl.program_id(0)
    plane = PlaneGather(n_ref, nall_ref, local, send, recv)
    depth = ZGather(xs_ref, xg_ref, zlocal, zsend, zrecv)
    gather_hooks(step, plane, depth)

    @pl.when(step == 0)
    def _():
        pk = across(rows(jnp.sum, n_ref[...].astype(F32) * el_ref[...].astype(F32)) * C2)
        pk_ref[...] = pk
        m_ref[...] = pk
        s_ref[...] = jnp.zeros_like(s_ref)
        acc_ref[...] = jnp.zeros_like(acc_ref)

    def run(count):
        n = n_ref[...]
        rel = lab_ref[...] - step * VBLK
        m = m_ref[:1, :]
        s = s_ref[:1, :]
        spans = [slice(lo, min(lo + VSUB, count)) for lo in range(0, count, VSUB)]
        ahead = dot(e_ref[spans[ONE], :], n, NT)
        for span, later in zip(spans, spans[1:] + [None]):
            l = ahead
            if later is not None:
                ahead = dot(e_ref[later, :], n, NT)
            new = jnp.maximum(m, cols(jnp.max, l) * C2)
            p = jnp.exp2(l * C2 - new)
            hit = lax.broadcasted_iota(jnp.int32, l.shape, 0) + span.start == rel
            p = jnp.where(hit, 0.0, p)
            alpha = jnp.exp2(m - new)
            s = s * alpha + cols(jnp.sum, p)
            acc_ref[...] = acc_ref[...] * alpha + dot(e_ref[span, :], p.astype(BF), TN)
            m = new
        m_ref[...] = jnp.broadcast_to(m, m_ref.shape)
        s_ref[...] = jnp.broadcast_to(s, s_ref.shape)

    @pl.when(step != VSTEPS - 1)
    def _():
        run(VBLK)

    @pl.when(step == VSTEPS - 1)
    def _():
        run(VOCAB % VBLK)
        m = m_ref[:1, :]
        s = s_ref[:1, :]
        pk = pk_ref[:1, :]
        total = s + jnp.exp2(pk - m)
        lse2 = m + jnp.log2(total)
        ce = (lse2 - pk) * (1.0 / LOG2E)
        row = lax.broadcasted_iota(jnp.int32, ids_ref.shape, 0)
        small = jnp.where(row == LSE, lse2, jnp.where(row == CE, ce, ids_ref[...]))
        small_ref[ONE] = small[:, :HSEQ]
        small_ref[OTHER] = small[:, HSEQ:]
        inv_total = 1.0 / total
        gn = jnp.transpose(acc_ref[...] * inv_total) - column(s * inv_total) * el_ref[...].astype(F32)
        gn = (gn * SCALE).astype(BF).astype(F32)
        wide = x2_ref[...].astype(F32)
        inv = inv_rms(wide)
        nw = wide * inv
        inner = rows(jnp.mean, gn * nw)
        gtop_ref[...] = (inv * (gn - nw * inner)).astype(BF)
        plane.go(4)
        depth.end()


def window_start(seg):
    owner = (seg * 4 + lax.axis_index('y')) * 4 + lax.axis_index('x')
    return jnp.minimum(owner * ROWS // 16 * 16, VOCAB - WIN)


def headgrad_kernel(table_ref, n_ref, all_ref, g0_ref, go_ref, out_ref, gall_ref, gg_ref, e_buf, sems,
                    local, send, recv, zlocal, zsend, zrecv):
    step = pl.program_id(0)
    plane = PlaneGather(g0_ref, gall_ref, local, send, recv)
    depth = ZGather(go_ref, gg_ref, zlocal, zsend, zrecv)

    def copy(seg):
        src = table_ref.at[pl.ds(pl.multiple_of(window_start(seg), 16), WIN), :]
        return pltpu.make_async_copy(src, e_buf.at[seg], sems.at[seg])

    @pl.when(step == 0)
    def _():
        for seg in SIDES:
            copy(seg).start()

    gather_hooks(step, plane, depth)

    @pl.when(step == 0)
    def _():
        out_ref[...] = jnp.zeros_like(out_ref)
        for seg in SIDES:
            copy(seg).wait()

    n = n_ref[...]
    def line(which):
        return jnp.concatenate([all_ref[ONE, ONE, q, pl.ds(which, 1), :] for q in SIDES], axis=1)

    lse = line(LSE) - math.log2(SCALE)
    lab = line(LAB).astype(jnp.int32)
    row = lax.broadcasted_iota(jnp.int32, (WIN, HBLK), 0)
    ahead = dot(e_buf[ONE], n, NT)
    for seg in SIDES:
        l = ahead
        if seg + 1 < len(SIDES):
            ahead = dot(e_buf[seg + 1], n, NT)
        p = jnp.exp2(l * C2 - lse)
        g = (p - jnp.where(row == lab - window_start(seg), SCALE, 0.0)).astype(BF)
        d = dot(g, n, NN)
        out_ref[seg, ONE] += d[:HALF]
        out_ref[seg, OTHER] += d[HALF:]

    @pl.when(step == HSTEPS - 1)
    def _():
        plane.go(4)
        depth.end()


def wgrad_kernel(xg_ref, gg_ref, up_ref, dn_ref, out_up, out_dn, wu, wd, acc_up, acc_dn, xbuf, gbuf, sems, xsems, gsems):
    iz = lax.axis_index('z')
    first = pl.multiple_of(iz * CHUNK, CHUNK)
    cu = pltpu.make_async_copy(up_ref.at[:, pl.ds(first, CHUNK)], wu, sems.at[ONE])
    cd = pltpu.make_async_copy(dn_ref.at[pl.ds(first, CHUNK), :], wd, sems.at[OTHER])
    loads = [(pltpu.make_async_copy(xg_ref.at[q], xbuf.at[q], xsems.at[q]), pltpu.make_async_copy(gg_ref.at[q], gbuf.at[q], gsems.at[q])) for q in SIDES]
    cu.start()
    cd.start()
    for copy in loads[ONE]:
        copy.start()
    cu.wait()
    for q in SIDES:
        for some in loads[q + 1:][:1]:
            for copy in some:
                copy.start()
        for copy in loads[q]:
            copy.wait()
        if q == ONE:
            cd.wait()
        x = xbuf[q].reshape(2 * SEQ, DIM)
        g = gbuf[q].reshape(2 * SEQ, DIM)
        hid = dot(x, wu[...], NN)
        gg = dot(g, wd[...], NT).astype(BF).astype(F32)
        gated = gelu(hid).astype(BF)
        gh = (gg * gelu_grad(hid)).astype(BF)
        du = dot(x, gh, TN)
        dd = dot(gated, g, TN)
        acc_up[...] = acc_up[...] + du if q else du
        acc_dn[...] = acc_dn[...] + dd if q else dd
    for kz, ky, kx in itertools.product(SIDES, SIDES, SIDES):
        out_up[kx, ky, pl.ds(URO * kz, URO), :] = acc_up[pl.ds(URO * ((kz * 4 + ky) * 4 + kx), URO), :]
    for ky, kx in itertools.product(SIDES, SIDES):
        out_dn[ky, kx] = acc_dn[pl.ds(DRO * (ky * 4 + kx), DRO), :]


class PlaneReduce:
    def __init__(self, src, first, second, bufs, sems):
        self.src, self.bufs, self.sems = src, bufs, sems
        self.first, self.second = first, second

    def axis(self, name):
        i = lax.axis_index(name)
        return i, mod4(i + 1), mod4(i - 1), mod4(i + 2)

    def sem(self, k):
        return pair(self.sems, k)

    def pieces(self, phase):
        rel1, fin1, snd1, total, rel2, fin2, snd2 = self.bufs
        if phase == 0:
            name, src, rel, fin, snd, half, base = self.first, self.src, rel1, fin1, snd1, 2, 0
        else:
            name, src, rel, fin, snd, half, base = self.second, total, rel2, fin2, snd2, 24, 6
        i, up, down, far = self.axis(name)
        lo, hi = pl.ds(0, half), pl.ds(half, half)
        to_up, to_down = {name: up}, {name: down}
        moves = ((src.at[far, lo], rel.at[ONE], to_up), (src.at[far, hi], rel.at[OTHER], to_down),
                 (src.at[up, hi], fin.at[ONE, hi], to_up), (src.at[down, lo], fin.at[OTHER, lo], to_down),
                 (snd.at[ONE], fin.at[ONE, lo], to_up), (snd.at[OTHER], fin.at[OTHER, hi], to_down))
        moves = [remote(a, b, *self.sem(base + k), **kw) for k, (a, b, kw) in enumerate(moves)]
        early, late = moves[:4], moves[4:]
        return i, up, down, lo, hi, src, rel, fin, snd, early, late

    def start(self, phase):
        for copy in self.pieces(phase)[-2]:
            copy.start()

    def relay(self, phase):
        i, up, down, lo, hi, src, rel, fin, snd, early, late = self.pieces(phase)
        for side, part in enumerate((src.at[up, lo], src.at[down, hi])):
            early[side].wait_recv()
            snd[side] = part[...] + rel[side]
            late[side].start()

    def finish(self, phase):
        i, up, down, lo, hi, src, rel, fin, snd, early, late = self.pieces(phase)
        for copy in early[2:] + late:
            copy.wait_recv()
        return src[i] + fin[ONE] + fin[OTHER]

    def drain(self, phase):
        early, late = self.pieces(phase)[-2:]
        for copy in early + late:
            copy.wait_send()


def final_kernel(part_hbm, g_hbm, all_ref, up_ref, dn_ref, tab_ref, upo_ref, dno_ref,
                 part_ref, g_ref, lsems, t_ref, swap_ref, zrel0, zrel1, zfin, mine, theirs, u4, ugot, *rest):
    bufs_a, bufs_b, (sems_a, sems_b, sems_c, sems_z, sems_u, sems_f) = rest[:7], rest[7:14], rest[14:]
    me, iz, iy, ix = (lax.axis_index(name) for name in ('stage', 'z', 'y', 'x'))
    up, down, far = mod4(iz + 1), mod4(iz - 1), mod4(iz + 2)
    order = (far, up, down, iz)
    load = pltpu.make_async_copy(g_hbm, g_ref, lsems.at[4])
    pieces = [pltpu.make_async_copy(part_hbm.at[seg], part_ref.at[k], lsems.at[k]) for k, seg in enumerate(order)]
    load.start()
    pieces[ONE].start()
    greet([dict(stage=1 - me), dict(z=up), dict(z=down), dict(z=far), dict(y=mod4(iy + 1)), dict(y=mod4(iy - 1)),
           dict(x=mod4(ix + 1)), dict(x=mod4(ix - 1))])
    red_a = PlaneReduce(up_ref, 'x', 'y', bufs_a, sems_a)
    red_b = PlaneReduce(dn_ref, 'y', 'x', bufs_b, sems_b)
    red_a.start(ONE)
    red_b.start(ONE)
    total_a, total_b = bufs_a[3], bufs_b[3]
    swaps = [remote(t_ref.at[seg, 1 - me], swap_ref.at[k], *pair(sems_c, k), stage=1 - me) for k, seg in enumerate(order)]
    lo, hi = pl.ds(0, SPLIT), pl.ds(SPLIT, HALF - SPLIT)

    to_up, to_down = dict(z=up), dict(z=down)
    moves = ((t_ref.at[far, me, lo], zrel0, to_up), (t_ref.at[far, me, hi], zrel1, to_down),
             (t_ref.at[up, me, hi], zfin.at[ONE, hi], to_up), (t_ref.at[up, me, lo], zfin.at[ONE, lo], to_up),
             (t_ref.at[down, me, lo], zfin.at[OTHER, lo], to_down), (t_ref.at[down, me, hi], zfin.at[OTHER, hi], to_down))
    moves = [remote(a, b, *pair(sems_z, k), **kw) for k, (a, b, kw) in enumerate(moves)]
    rel_up, rel_down, up_hi, up_lo, down_lo, down_hi = moves

    def embed(k, half):
        seg = order[k]
        row = lax.broadcasted_iota(jnp.int32, (HALF, TBLK), 0) + (window_start(seg) + half * HALF)
        for b in SIDES:
            blocks = [divmod(SUBL * b + q, 4) for q in range(SUBL)]
            tok = jnp.concatenate([all_ref[i // 4, i % 4, q, pl.ds(TOK, 1), :] for i, q in blocks], axis=1).astype(jnp.int32)
            hot = jnp.where(row == tok, 1.0, 0.0).astype(BF)
            d = dot(hot, g_ref[b * TBLK:(b + 1) * TBLK, :], NN)
            base = t_ref.at[seg] if b else part_ref.at[k]
            t_ref[seg, half] = base[half] + d

    def settle(k):
        pieces[k].wait()
        embed(k, 1 - me)
        swaps[k].start()
        embed(k, me)
        swaps[k].wait_recv()
        t_ref[order[k], me] += swap_ref[k]

    ifar, iup, idown, iown = SIDES
    load.wait()
    for copy in pieces[1:]:
        copy.start()
    settle(ifar)
    rel_up.start()
    rel_down.start()
    settle(iup)
    up_hi.start()
    red_a.relay(ONE)
    red_b.relay(ONE)
    settle(idown)
    down_lo.start()
    rel_up.wait_recv()
    t_ref[up, me, lo] += zrel0[...]
    up_lo.start()
    rel_down.wait_recv()
    t_ref[down, me, hi] += zrel1[...]
    down_hi.start()
    settle(iown)
    total_a[...] = red_a.finish(ONE)
    red_a.start(OTHER)
    total_b[...] = red_b.finish(ONE)
    red_b.start(OTHER)
    red_a.relay(OTHER)
    red_b.relay(OTHER)
    total = red_a.finish(OTHER)
    for k in SIDES:
        u4[k] = total[URO * k:URO * (k + 1), :]
    turns = [remote(u4.at[mod4(iz + k)], ugot.at[iz], *pair(sems_u, k), z=mod4(iz + k)) for k in SIDES[1:]]
    for copy in turns:
        copy.start()
    dno_ref[...] = red_b.finish(OTHER)
    for copy in (up_hi, up_lo, down_lo, down_hi):
        copy.wait_recv()
    mine[...] = t_ref[iz, me] + zfin[ONE] + zfin[OTHER]
    back = remote(mine, theirs, sems_f.at[ONE], sems_f.at[OTHER], stage=1 - me)
    back.start()
    tab_ref[me] = mine[...]
    for copy in turns:
        copy.wait_recv()
    upo_ref[...] = ugot[...]
    upo_ref[iz] = u4[iz]
    back.wait_recv()
    tab_ref[1 - me] = theirs[...]
    for copy in swaps + moves + [back] + turns:
        copy.wait_send()
    for phase in (ONE, OTHER):
        red_a.drain(phase)
        red_b.drain(phase)


def cost(flops, nbytes, trans=0):
    return pl.CostEstimate(flops=int(flops), bytes_accessed=int(nbytes), transcendentals=int(trans))


def vmem(n):
    return [pl.BlockSpec(memory_space=pltpu.VMEM)] * n


def shape(dims, dtype=F32):
    return jax.ShapeDtypeStruct(dims, dtype)


def comm(cid):
    return pltpu.CompilerParams(collective_id=cid, has_side_effects=True)


WBUFS = [pltpu.VMEM((2, NCH, DIM, CHUNK), BF), pltpu.VMEM((2, NCH, CHUNK, DIM), BF), pltpu.SemaphoreType.DMA((2, NCH, 2)),
         pltpu.VMEM((2, NCH, SEQ, CHUNK), F32), pltpu.SemaphoreType.DMA((2, NCH))]
HID = (2, NCH, SEQ, CHUNK)
GSEMS = [pltpu.SemaphoreType.DMA((2,)), pltpu.SemaphoreType.DMA((32,)), pltpu.SemaphoreType.DMA((32,)),
         pltpu.SemaphoreType.DMA, pltpu.SemaphoreType.DMA((5,)), pltpu.SemaphoreType.DMA((5,))]
PLANE = (2, 4, 4, SEQ // 2, DIM)
SMALL = (2, 4, 4, 8, SEQ // 2)


def call_fwd(x, *weights):
    tok = shape((SEQ, DIM), BF)
    dma = pltpu.SemaphoreType.DMA
    return pl.pallas_call(
        fwd_kernel,
        out_shape=(shape((2, SEQ, DIM), BF), tok, tok, shape(HID), shape((FFN, DIM), BF)),
        in_specs=vmem(1) + [any_spec()] * 3,
        out_specs=vmem(3) + [any_spec()] * 2,
        scratch_shapes=WBUFS + [dma((NCH,))] * 3,
        compiler_params=comm(5),
        cost_estimate=cost(8 * SEQ * DIM * FFN, 26e6),
        name='fwd')(x, *weights)


def call_bwd(g, h, small, *weights):
    return pl.pallas_call(
        bwd_kernel,
        out_shape=(shape((2, SEQ, DIM), BF), shape((SEQ, DIM), BF), shape(SMALL), shape((2, 2, 8, HSEQ))),
        in_specs=vmem(1) + [any_spec()] + vmem(1) + [any_spec()] * 4,
        out_specs=vmem(4),
        scratch_shapes=WBUFS + [pltpu.SemaphoreType.DMA((2, 16)), pltpu.SemaphoreType.DMA((2, 16))],
        compiler_params=comm(1),
        cost_estimate=cost(8 * SEQ * DIM * FFN, 26e6),
        name='bwd')(g, h, small, *weights)


def call_head(n, lab, ids, el, x2, xs, table):
    return pl.pallas_call(
        head_kernel,
        grid=(VSTEPS,),
        out_shape=(shape((SEQ, DIM), BF), shape((2, 8, HSEQ)), shape(PLANE, BF), shape((4, 2, SEQ, DIM), BF)),
        in_specs=[whole((SEQ, DIM)), whole((1, SEQ)), whole((8, SEQ)), whole((SEQ, DIM)), whole((SEQ, DIM)), whole((2, SEQ, DIM)),
                  pl.BlockSpec((VBLK, DIM), lambda i: (i, 0))],
        out_specs=(whole((SEQ, DIM)), whole((2, 8, HSEQ)), any_spec(), any_spec()),
        scratch_shapes=[pltpu.VMEM((DIM, SEQ), F32)] + [pltpu.VMEM((8, SEQ), F32)] * 3 + GSEMS,
        compiler_params=comm(2),
        cost_estimate=cost(4 * SEQ * DIM * VOCAB, VOCAB * DIM * 2, SEQ * VOCAB),
        name='head')(n, lab, ids, el, x2, xs, table)


def call_headgrad(table, n_all, small_all, g0, go):
    toks = 16 * SEQ
    return pl.pallas_call(
        headgrad_kernel,
        grid=(HSTEPS,),
        out_shape=(shape((4, 2, HALF, DIM)), shape(PLANE, BF), shape((4, 2, SEQ, DIM), BF)),
        in_specs=[any_spec(), pl.BlockSpec((HBLK, DIM), lambda i: (i, 0)),
                  pl.BlockSpec((1, 1, 4, 8, HSEQ), lambda i: (i // 4, i % 4, 0, 0, 0)), whole((SEQ, DIM)), whole((2, SEQ, DIM))],
        out_specs=(whole((4, 2, HALF, DIM)), any_spec(), any_spec()),
        scratch_shapes=[pltpu.VMEM((4, WIN, DIM), BF), pltpu.SemaphoreType.DMA((4,))] + GSEMS,
        compiler_params=comm(3),
        cost_estimate=cost(4 * 4 * WIN * DIM * toks, 16e6, 4 * WIN * toks),
        name='headgrad')(table, n_all.reshape(toks, DIM), small_all, g0, go)


def call_wgrad(xg, gg, own_up, own_dn):
    dma = pltpu.SemaphoreType.DMA
    tokens = pltpu.VMEM((4, 2, SEQ, DIM), BF)
    return pl.pallas_call(
        wgrad_kernel,
        out_shape=(shape((4, 4, DRO, DIM)), shape((4, 4, DRO, DIM))),
        in_specs=[any_spec()] * 4,
        out_specs=vmem(2),
        scratch_shapes=[pltpu.VMEM((DIM, CHUNK), BF), pltpu.VMEM((CHUNK, DIM), BF), pltpu.VMEM((DIM, CHUNK), F32),
                        pltpu.VMEM((CHUNK, DIM), F32), tokens, tokens, dma((2,)), dma((4,)), dma((4,))],
        cost_estimate=cost(8 * 2048 * DIM * CHUNK, 16e6),
        name='wgrad')(xg, gg, own_up, own_dn)


def plane_bufs():
    return [pltpu.VMEM((2, 2, DRO, DIM), F32), pltpu.VMEM((2, 4, DRO, DIM), F32), pltpu.VMEM((2, 2, DRO, DIM), F32),
            pltpu.VMEM((4, DRO, DIM), F32), pltpu.VMEM((2, 24, DIM), F32), pltpu.VMEM((2, DRO, DIM), F32), pltpu.VMEM((2, 24, DIM), F32)]


def call_final(part, g_all, small_all, d_up, d_dn):
    dma = pltpu.SemaphoreType.DMA
    return pl.pallas_call(
        final_kernel,
        out_shape=(shape((2, HALF, DIM)), shape((4, URO, DIM)), shape((DRO, DIM))),
        in_specs=[any_spec()] * 2 + vmem(3),
        out_specs=vmem(3),
        scratch_shapes=[pltpu.VMEM((4, 2, HALF, DIM), F32), pltpu.VMEM((16 * SEQ, DIM), BF), dma((6,)), pltpu.VMEM((4, 2, HALF, DIM), F32), pltpu.VMEM((4, HALF, DIM), F32), pltpu.VMEM((SPLIT, DIM), F32),
                        pltpu.VMEM((HALF - SPLIT, DIM), F32), pltpu.VMEM((2, HALF, DIM), F32), pltpu.VMEM((HALF, DIM), F32),
                        pltpu.VMEM((HALF, DIM), F32), pltpu.VMEM((4, URO, DIM), F32), pltpu.VMEM((4, URO, DIM), F32)]
        + plane_bufs() + plane_bufs() + [dma((2, URO)), dma((2, URO)), dma((2, SUBL)), dma((2, SUBL)), dma((2, SUBL)), dma((2,))],
        compiler_params=comm(4),
        cost_estimate=cost(2 * 4 * WIN * DIM * 4096, 20e6),
        name='final')(part, g_all.reshape(16 * SEQ, DIM), small_all, d_up, d_dn)


SWAP = [(0, 1), (1, 0)]


def step_program(token_rows, label_rows, table, up_block, down_block):
    me = lax.axis_index('stage')
    iz, iy, ix = lax.axis_index('z'), lax.axis_index('y'), lax.axis_index('x')
    own_up, own_dn = up_block[0], down_block[0]
    oth_up = lax.ppermute(own_up, 'stage', SWAP)
    tok = lax.dynamic_index_in_dim(token_rows, me, 0, keepdims=False)
    lab = lax.dynamic_index_in_dim(label_rows, me, 0, keepdims=False)
    ids = jnp.concatenate([lab[None], lab[None]] + [tok[None]] * 6, axis=0).astype(F32)
    rows = table[jnp.concatenate([tok, lab])]
    x0, el = rows[:SEQ], rows[SEQ:]
    xs, x2, n, h, oth_dn = call_fwd(x0, own_up, own_dn, oth_up)
    weights = (own_up, own_dn, oth_up, oth_dn)
    gtop, small, n_all, xg = call_head(n, lab[None], ids, el, x2, xs, table)
    go, g0, small_all, pair = call_bwd(gtop, h, small, *weights)
    part, g_all, gg = call_headgrad(table, n_all, small_all, g0, go)
    d_up, d_dn = call_wgrad(xg, gg, own_up, own_dn)
    both, up_parts, grad_down = call_final(part, g_all, small_all, d_up, d_dn)
    grad_up = up_parts.transpose(1, 0, 2).reshape(1, URO, FFN)
    owner = (iz * 4 + iy) * 4 + ix
    begin = jnp.minimum(owner * ROWS // 16 * 16, VOCAB - WIN)
    grad_table = lax.dynamic_slice_in_dim(both.reshape(WIN, DIM), owner * ROWS - begin, ROWS, 0)
    losses = jnp.mean(pair[:, :, 3, :], axis=(1, 2))
    return losses, grad_table, grad_up, grad_down[None]


def solution(mesh):
    fine = jax.sharding.Mesh(mesh.devices.reshape(1, 4, 4, 4, 2), AXES)
    data = ('z', 'y', 'x')
    rows_spec = P(('pod',) + data, None)
    return jax.shard_map(step_program, mesh=fine,
                         in_specs=(rows_spec, rows_spec, P(None, None), P('stage', None, None), P('stage', None, None)),
                         out_specs=(P(('pod',) + data), rows_spec, P(('pod', 'stage'), data, None), P(('pod', 'stage'), data, None)),
                         check_vma=False)
```
